256 devices in a mesh: band: 8 (over y, core), col: 32 (over z, x).
Axes of the slice: x: 4, y: 4, z: 8, core: 2. Of those that a mesh axis runs over, the one named last changes fastest.
Arguments:
- source: bfloat16 [6, 4194304], P(None, ('band', 'col')), may hold values from -6 to 6
- weights: bfloat16 [65536, 128, 128], P(('band', 'col')), may hold values from -0.5 to 0.5
- source_block: int32 [65536], P(('band', 'col')), may hold values from 0 to 127
- owner_device: int32 [65536, 1], P(('band', 'col')), may hold values from 0 to 255, as said below
- target_tile: int32 [65536], P(('band', 'col')), may hold values from 0 to 112, as said below
- cutoff: int32 [512], P(('band', 'col')), may hold values from 1 to 511
Outputs:
- remapped: float32 [6, 512, 7200], P(None, 'band', 'col')
- filtered: float32 [6, 512, 7200], P(None, 'band', 'col')
The draws below stay inside these ranges and needn't reach their ends.
Inputs may be any that keep to these rules, and one draw needn't show every extreme that they name: `owner_device`: owners are numbered band index times 32 plus col index. A device's blocks go only to owners in its own band or in the bands next to it. Among the 256 blocks of one device at most 6 share an owner; in every device exactly 6 do for some owner of its own band, and exactly 6 for some owner of each band next to its own; every device sends at least 4 blocks to each owner of its own band. `target_tile`: every tile of every owner receives at least one block.
All inputs are finite; a program needn't handle non-finite values.
Results may differ from the reference program's by a relative error of at most 0.0003.
Values sent between devices are 32-bit elements; how exact they have to be, the bound alone decides.
A program may use at most 64 MiB of HBM per device.

```python
import jax
import jax.numpy as jnp
from jax import lax

NLON = 7200
BLK = 128
LEV = 6
KW = 512
NB = 256
SB = 128
LATB = 64
NLAT = 512
LON_DEV = 225
TILES_DEV = 113
REG = 4
CAP = 6
NBLOCKS = 65536
NSRC = 4194304
N_BAND = 8
N_COL = 32
DEVICES = 256


def remap_layout(key):
    slot_total = 3 * N_COL * CAP
    slots = jnp.arange(slot_total, dtype=jnp.int32)
    offset = slots // (N_COL * CAP)
    owner_col = slots // CAP % N_COL
    within = slots % CAP
    shifts = jax.random.randint(jax.random.fold_in(key, 11), (DEVICES,), 0, TILES_DEV).astype(jnp.int32)

    def one_device(device):
        device_key = jax.random.fold_in(jax.random.fold_in(key, 17), device)
        band = device // N_COL
        column = device % N_COL
        owner_band = band + offset - 1
        valid = (owner_band >= 0) & (owner_band < N_BAND)
        regular = (offset == 1) & (within < REG)
        candidate = valid & ((offset != 1) | (within >= REG))
        forced_cols = jax.random.randint(jax.random.fold_in(device_key, 1), (3,), 0, N_COL).astype(jnp.int32)
        forced = candidate & (owner_col == forced_cols[offset])
        ranking = jax.random.permutation(jax.random.fold_in(device_key, 2), slot_total).astype(jnp.int32)
        score = jnp.where(regular, 0, jnp.where(forced, 1, jnp.where(candidate, 2 + ranking, 4 * slot_total + 4)))
        chosen = jnp.argsort(score, stable=True)[:NB].astype(jnp.int32)
        mixing = jax.random.permutation(jax.random.fold_in(device_key, 3), NB).astype(jnp.int32)
        chosen = chosen[mixing]
        owners = (owner_band[chosen] * N_COL + owner_col[chosen]).astype(jnp.int32)
        random_tile = jax.random.randint(jax.random.fold_in(device_key, 4), (NB,), 0, TILES_DEV).astype(jnp.int32)
        regular_tile = (column * REG + within[chosen] + shifts[owners]) % TILES_DEV
        tiles = jnp.where(regular[chosen], regular_tile, random_tile).astype(jnp.int32)
        return (owners, tiles)
    owners, tiles = jax.vmap(one_device)(jnp.arange(DEVICES, dtype=jnp.int32))
    return (owners.reshape(NBLOCKS, 1).astype(jnp.int32), tiles.reshape(NBLOCKS).astype(jnp.int32))


def draw_owner_device(key, part):
    return remap_layout(jax.random.fold_in(key, 5))[0]


def draw_target_tile(key, part):
    return remap_layout(jax.random.fold_in(key, 5))[1]


def place_ends(array, key, low, high):
    place = [jax.random.randint(jax.random.fold_in(key, axis), (), 0, length) for axis, length in enumerate(array.shape)]
    longest = array.shape.index(max(array.shape))
    beside = place[:longest] + [(place[longest] + 1) % array.shape[longest]] + place[longest + 1:]
    return array.at[tuple(place)].set(low).at[tuple(beside)].set(high)


def levels(rng, dims, pieces, low, largest):
    factor_of, own = 1.0, jax.random.fold_in(rng, 6)
    for position, parts in pieces:
        draws = jnp.exp(jax.random.uniform(jax.random.fold_in(own, position), (parts,), jnp.float32, low / len(pieces), largest / len(pieces)))
        factor_of = factor_of * jnp.repeat(draws, dims[position] // parts).reshape([-1 if axis == position else 1 for axis in range(len(dims))])
    return factor_of


def centred(own_key, dims, width, most, split=(), kind=jnp.bfloat16):
    gain = levels(own_key, dims, split, -0.22, 0.18) if split else 1.0
    result = jax.random.normal(own_key, dims, jnp.float32) * width * gain
    return jnp.minimum(jnp.maximum(result, -most), most).astype(kind)


def setup_inputs(seed: int = 0) -> dict:
    splits = jax.random.split(jax.random.key(seed), 7)
    source = centred(splits[0], (LEV, NSRC), 1.0, 6.0, ((1, 256),))
    weights = centred(splits[1], (NBLOCKS, BLK, BLK), BLK ** -0.5, 0.5, ((0, 256),))
    source_block = place_ends(jax.random.randint(splits[2], (NBLOCKS,), 0, SB), jax.random.fold_in(splits[2], 1), 0, SB - 1).astype(jnp.int32)
    owner_device = draw_owner_device(jax.random.fold_in(splits[6], 71), 0)
    target_tile = draw_target_tile(jax.random.fold_in(splits[6], 71), 0)
    cutoff = place_ends(jax.random.randint(splits[5], (NLAT,), 1, KW), jax.random.fold_in(splits[5], 1), 1, KW - 1).astype(jnp.int32)
    return {"source": source, "weights": weights, "source_block": source_block, "owner_device": owner_device, "target_tile": target_tile, "cutoff": cutoff}


TWO_PI = 6.283185307179586


def zonal_table(start_index, length, period, wave_count):
    positions = start_index + lax.broadcasted_iota(jnp.int32, (length, wave_count), 0)
    wave_index = lax.broadcasted_iota(jnp.int32, (length, wave_count), 1)
    phases = (positions * wave_index) % period
    angles = phases.astype(jnp.float32) * (TWO_PI / period)
    return jnp.concatenate([jnp.cos(angles), jnp.sin(angles)], axis=1)


def spectral_weights(cutoffs, wave_count, period):
    wave_index = lax.broadcasted_iota(jnp.int32, (cutoffs.shape[0], wave_count), 1)
    scaled = jnp.where(wave_index == 0, 1.0, 2.0) / period
    retained = jnp.where(wave_index <= cutoffs[:, None], scaled, 0.0).astype(jnp.float32)
    return jnp.concatenate([retained, retained], axis=1)


def reference(source, weights, source_block, owner_device, target_tile, cutoff):
    device_total = N_BAND * N_COL
    blocks_all = source.reshape(LEV, device_total * SB, BLK)
    owners_all = owner_device[:, 0]

    def add_device(totals, device_index):
        first_block = device_index * NB
        block_weights = lax.dynamic_slice_in_dim(weights, first_block, NB, 0)
        chosen = lax.dynamic_slice_in_dim(source_block, first_block, NB, 0)
        owners = lax.dynamic_slice_in_dim(owners_all, first_block, NB, 0)
        tiles_hit = lax.dynamic_slice_in_dim(target_tile, first_block, NB, 0)
        picked = jnp.take(blocks_all, (device_index * SB + chosen).astype(jnp.int32), axis=1)
        partial_value = jnp.einsum("lnb,nbt->nlt", picked.astype(jnp.float32), block_weights.astype(jnp.float32))
        totals = totals.at[(owners * TILES_DEV + tiles_hit).astype(jnp.int32)].add(partial_value)
        return totals, None

    totals, unused = lax.scan(add_device, jnp.zeros((device_total * TILES_DEV, LEV, BLK), jnp.float32), jnp.arange(device_total, dtype=jnp.int32))
    cell_count = LATB * LON_DEV
    tiles = totals.reshape(N_BAND, N_COL, TILES_DEV, LEV, BLK)
    tiles = jnp.transpose(tiles, (3, 0, 1, 2, 4)).reshape(LEV, N_BAND, N_COL, TILES_DEV * BLK)[:, :, :, :cell_count]
    tiles = tiles.reshape(LEV, N_BAND, N_COL, LATB, LON_DEV)
    remapped = jnp.transpose(tiles, (0, 1, 3, 2, 4)).reshape(LEV, NLAT, NLON)
    wave_table = zonal_table(0, NLON, NLON, KW)
    spectrum = jnp.dot(remapped.reshape(LEV * NLAT, NLON), wave_table, precision=lax.Precision.HIGHEST, preferred_element_type=jnp.float32)
    spectrum = spectrum.reshape(LEV, NLAT, 2 * KW) * spectral_weights(cutoff, KW, NLON)[None]
    filtered = jnp.dot(spectrum.reshape(LEV * NLAT, 2 * KW), wave_table.T, precision=lax.Precision.HIGHEST, preferred_element_type=jnp.float32)
    return remapped, filtered.reshape(LEV, NLAT, NLON)
```

```python
import functools
import math

import jax
import jax.numpy as jnp
from jax import lax
from jax.experimental import pallas as pl
from jax.experimental.pallas import tpu as pltpu
from jax.sharding import PartitionSpec as P

NLON = 7200
KW = 512
CAP = 6
ROWS = 40
SENT = 37
TWO_PI = 6.283185307179586
MESH = pl.DeviceIdType.MESH
F32 = jnp.float32
BF16 = jnp.bfloat16
NZ, NX = 8, 4


def real_dft(xs):
    n = len(xs)
    if n == 1:
        return [(xs[0], None)]
    if n == 2:
        return [(xs[0] + xs[1], None), (xs[0] - xs[1], None)]
    even, odd = real_dft(xs[0::2]), real_dft(xs[1::2])
    half = n // 2

    def entry(spec, r):
        if r <= half // 2:
            re, im = spec[r]
            return re, im
        re, im = spec[half - r]
        return re, (None if im is None else -im)

    out = []
    for r in range(half + 1):
        if r == half:
            out.append((even[0][0] - odd[0][0], None))
            continue
        er, ei = entry(even, r)
        o_r, oi = entry(odd, r)
        if r == 0:
            out.append((er + o_r, None))
            continue
        if 4 * r == n:
            re = er if oi is None else er + oi
            im = -o_r if ei is None else ei - o_r
            out.append((re, im))
            continue
        c, s = math.cos(2 * math.pi * r / n), math.sin(2 * math.pi * r / n)
        if oi is None:
            tr, ti = c * o_r, -s * o_r
        else:
            tr, ti = c * o_r + s * oi, c * oi - s * o_r
        out.append((er + tr, ti if ei is None else ei + ti))
    return out


def real_idft(hs, n):
    if n == 1:
        return [hs[0][0]]
    if n == 2:
        return [hs[0][0] + hs[1][0], hs[0][0] - hs[1][0]]
    half = n // 2
    evens, odds = [], []
    for r in range(half // 2 + 1):
        re, im = hs[r]
        mr, mi = hs[half - r]
        sum_re, dif_re = re + mr, re - mr
        if r == 0:
            evens.append((sum_re, None))
            odds.append((dif_re, None))
            continue
        if 2 * r == half:
            evens.append((sum_re, None))
            odds.append((-2.0 * im, None))
            continue
        sum_im, dif_im = im - mi, im + mi
        c, s = math.cos(2 * math.pi * r / n), math.sin(2 * math.pi * r / n)
        evens.append((sum_re, sum_im))
        odds.append((c * dif_re - s * dif_im, c * dif_im + s * dif_re))
    a, b = real_idft(evens, half), real_idft(odds, half)
    out = []
    for x, y in zip(a, b):
        out += [x, y]
    return out


def halves(x):
    hi = x.astype(BF16)
    return hi, (x - hi.astype(F32)).astype(BF16)


def fill_tables(base_ref, table):
    ca, sa = base_ref[0:16, :], base_ref[16:32, :]
    for r in range(17):
        parts = []
        for k, sign in ((r, 1.0), (32 - r, -1.0)):
            cb = base_ref[32 + k : 33 + k, :]
            sb = base_ref[72 + k : 73 + k, :]
            c = ca * cb - sa * sb
            s = sa * cb + ca * sb
            parts.append((c, s, sign))
        for p, (c, s, sign) in enumerate(parts):
            for row, half, value in (
                (32 * p, 0, c),
                (32 * p, 1, sign * s),
                (32 * p + 16, 0, -s),
                (32 * p + 16, 1, sign * c),
            ):
                hi, lo = halves(value)
                table[0, r, row : row + 16, 256 * half : 256 * half + 256] = hi
                table[1, r, row : row + 16, 256 * half : 256 * half + 256] = lo


def zonal(rows_ref, out_ref, table, scale_ref):
    spec = real_dft([rows_ref[c] for c in range(32)])
    nt = (((1,), (1,)), ((), ()))
    nn = (((1,), (0,)), ((), ()))

    def widen(y):
        v0, v1, v2 = y[0:8], y[8:16], y[16:24]
        rolled = jnp.concatenate([v1[4:8], v1[0:4]], axis=0)
        return jnp.concatenate(
            [jnp.concatenate([v0, v1], axis=0), jnp.concatenate([v2, rolled], axis=0)], axis=1
        )

    def narrow(w):
        a, b = w[:, 0:128], w[:, 128:256]
        mid = jnp.concatenate([a[8:12], b[8:12]], axis=0)
        return jnp.concatenate([a[0:8], mid, b[0:8]], axis=0)

    back = []
    for r in range(17):
        re, im = spec[r]
        re = widen(re)
        im = jnp.zeros_like(re) if im is None else widen(im)
        hi, lo = halves(jnp.concatenate([re, im], axis=1))
        both = jnp.concatenate([hi, lo], axis=0)
        p = lax.dot_general(both, table[0, r], nt, preferred_element_type=F32)
        q = lax.dot_general(hi, table[1, r], nt, preferred_element_type=F32)
        s = (p[0:16] + p[16:32] + q) * scale_ref[r]
        hi, lo = halves(s)
        both = jnp.concatenate([hi, lo], axis=0)
        p = lax.dot_general(both, table[0, r], nn, preferred_element_type=F32)
        q = lax.dot_general(hi, table[1, r], nn, preferred_element_type=F32)
        w = p[0:16] + p[16:32] + q
        back.append((narrow(w[:, 0:256]), None if r in (0, 16) else narrow(w[:, 256:512])))
    for c, value in enumerate(real_idft(back, 32)):
        out_ref[c] = value


def exchange_kernel(sb_ref, id_ref, part_ref, out_ref, send, recv, data, send_sem, recv_sem):
    bands = lax.axis_size("band")
    band, col = lax.axis_index("band"), lax.axis_index("col")
    z, x = col // NX, lax.rem(col, NX)
    cols = NZ * NX

    def peer(i):
        u, dx = i // NX, lax.rem(i, NX)
        m = (u + 1) // 2
        dz = jnp.where(lax.rem(u, 2) == 0, 4 + m, 4 - m)
        return lax.rem(z + dz, NZ) * NX + lax.rem(x + dx, NX)

    def targets(act):
        def step(i, carry):
            to = peer(i)
            for off in (0, 2, 1):
                other = band + off - 1
                if off == 1:
                    ok = to != col
                else:
                    ok = (other >= 0) & (other < bands)

                @pl.when(ok)
                def _(off=off, other=other):
                    act(off, other, to)

            return carry

        lax.fori_loop(0, cols, step, 0)

    barrier = pltpu.get_barrier_semaphore()
    targets(lambda off, b, c: pl.semaphore_signal(barrier, inc=1, device_id=(b, c), device_id_type=MESH))

    for side, edge in ((0, 0), (2, bands - 1)):

        @pl.when(band == edge)
        def _(side=side):
            recv[side] = jnp.full(recv.shape[1:], -1.0, F32)

    def pack(j, carry):
        off, c = j // cols, lax.rem(j, cols)
        for s in range(CAP):
            block = sb_ref[j * CAP + s]
            send[off, c, pl.ds(s, 6, stride=CAP), :] = part_ref[block]
        send[off, c, 36:37, :] = id_ref[pl.ds(j, 1), :]
        return carry

    lax.fori_loop(0, 3 * cols, pack, 0)
    inner = (band > 0).astype(jnp.int32) + (band < bands - 1).astype(jnp.int32)
    pl.semaphore_wait(barrier, cols - 1 + cols * inner)

    def start(off, b, c):
        pltpu.make_async_remote_copy(
            src_ref=send.at[off, c, 0:SENT],
            dst_ref=recv.at[2 - off, col, 0:SENT],
            send_sem=send_sem.at[off],
            recv_sem=recv_sem.at[2 - off],
            device_id=(b, c),
            device_id_type=MESH,
        ).start()

    targets(start)
    own = pltpu.make_async_copy(send.at[1, col, 0:SENT], recv.at[1, col, 0:SENT], recv_sem.at[1])
    own.start()
    data[...] = jnp.zeros_like(data)

    def drain(off):
        pltpu.make_async_copy(recv.at[off, :, 0:SENT], recv.at[off, :, 0:SENT], recv_sem.at[off]).wait()

    def drain_send(off, n):
        pltpu.make_async_copy(
            send.at[off, 0:n, 0:SENT], send.at[off, 0:n, 0:SENT], send_sem.at[off]
        ).wait()

    drain(1)
    drain_send(1, cols - 1)
    for off in (0, 2):
        other = band + off - 1

        @pl.when((other >= 0) & (other < bands))
        def _(off=off):
            drain(off)
            drain_send(off, cols)

    for off in range(3):

        def lay(c, carry, off=off):
            j = off * cols + c
            for lev in range(6):
                data[pl.ds(pl.multiple_of(j * 8, 8), 6), 128 * lev : 128 * lev + 128] = recv[
                    off, c, lev * CAP : lev * CAP + CAP, :
                ]
            return carry

        lax.fori_loop(0, cols, lay, 0)
    ids = recv[:, :, 36:37, :].reshape(3 * cols, 1, 128)
    lane = lax.broadcasted_iota(jnp.int32, (3 * cols, 8, 128), 2)
    sub = lax.broadcasted_iota(jnp.int32, (3 * cols, 8, 128), 1)
    diag = jnp.where(lane == sub, jnp.broadcast_to(ids, (3 * cols, 8, 128)), 0.0)
    diag = diag.reshape(24 * cols, 128).astype(BF16)
    spread = jnp.dot(diag, jnp.ones((128, 128), BF16), preferred_element_type=F32)
    tile = lax.broadcasted_iota(jnp.int32, (24 * cols, 128), 1).astype(F32)
    chooser = (spread == tile).astype(F32).astype(BF16)
    hi, lo = halves(data[...])
    tn = (((0,), (0,)), ((), ()))
    out_ref[...] = lax.dot_general(chooser, hi, tn, preferred_element_type=F32) + lax.dot_general(
        chooser, lo, tn, preferred_element_type=F32
    )


def zonal_kernel(base_ref, scale_ref, rows_ref, out_ref, table):
    fill_tables(base_ref, table)
    zonal(rows_ref, out_ref, table, scale_ref)


def base_tables():
    i = lax.broadcasted_iota(jnp.int32, (112, 256), 1)
    row = lax.broadcasted_iota(jnp.int32, (112, 256), 0)
    k = jnp.where(row < 32, 32 * (row % 16), (row - 32) % 40)
    angle = ((i * k) % NLON).astype(F32) * (TWO_PI / NLON)
    is_sin = ((row >= 16) & (row < 32)) | (row >= 72)
    value = jnp.where(is_sin, jnp.sin(angle), jnp.cos(angle))
    return jnp.where(i < 225, value, 0.0)


def scales(cutoff):
    r = lax.broadcasted_iota(jnp.int32, (17, 16, 64), 0)
    row = lax.broadcasted_iota(jnp.int32, (17, 16, 64), 1)
    n = lax.broadcasted_iota(jnp.int32, (17, 16, 64), 2)
    mirror = n >= 32
    k = 32 * (n % 16) + jnp.where(mirror, 32 - r, r)
    used = (~mirror) | ((r > 0) & (r < 16))
    weight = jnp.where((k > 0) & ((r == 0) | (r == 16)), 2.0, 1.0) / NLON
    limit = jnp.where(row < 6, cutoff[0], cutoff[1])
    return jnp.where(used & (k <= limit), weight, 0.0).astype(F32)


def to_chunk(a):
    a = jnp.pad(a.reshape(32, 12, 225), ((0, 0), (0, 0), (0, 31)))
    first, second = a[:, :, :128], a[:, :, 128:]
    return jnp.concatenate([first, second[:, 8:12], second[:, 0:8]], axis=1)


def from_chunk(a):
    second = jnp.concatenate([a[:, 16:24], a[:, 12:16]], axis=1)
    return jnp.concatenate([a[:, :12], second], axis=2)[:, :, :225].reshape(32, 2, 6, 225)


def local(source, weights, source_block, owner_device, target_tile, cutoff):
    cols = lax.axis_size("col")
    levels, nb, width = 6, weights.shape[0], weights.shape[1]
    band = lax.axis_index("band")
    picked = jnp.take(source.reshape(levels, -1, width), source_block, axis=1)
    partial = jnp.einsum("lnb,nbt->nlt", picked, weights, preferred_element_type=F32)
    owners = owner_device[:, 0]
    row = lax.broadcasted_iota(jnp.int32, (nb, nb), 0)
    column = lax.broadcasted_iota(jnp.int32, (nb, nb), 1)
    earlier = (owners[None, :] == owners[:, None]) & (column < row)
    rank = jnp.sum(earlier.astype(jnp.int32), axis=1)
    slot = (owners - (band - 1) * cols) * CAP + rank
    total = 3 * cols * CAP
    hit = lax.broadcasted_iota(jnp.int32, (total, nb), 0) == slot[None, :]
    both = jnp.arange(nb, dtype=jnp.int32) * 128 + target_tile
    code = jnp.sum(jnp.where(hit, both[None, :] + 1, 0), axis=1)
    sb = jnp.maximum(code - 1, 0) // 128
    tid = jnp.where(code > 0, (code - 1) % 128, -1).astype(F32)
    id_rows = jnp.pad(tid.reshape(3 * cols, CAP), ((0, 0), (0, 128 - CAP)), constant_values=-1.0)
    vmem = pl.BlockSpec(memory_space=pltpu.VMEM)
    summed = pl.pallas_call(
        exchange_kernel,
        name="exchange",
        out_shape=jax.ShapeDtypeStruct((128, 768), F32),
        in_specs=[pl.BlockSpec(memory_space=pltpu.SMEM), vmem, vmem],
        out_specs=vmem,
        scratch_shapes=[
            pltpu.VMEM((3, cols, ROWS, 128), F32),
            pltpu.VMEM((3, cols, ROWS, 128), F32),
            pltpu.VMEM((24 * cols, 768), F32),
            pltpu.SemaphoreType.DMA((3,)),
            pltpu.SemaphoreType.DMA((3,)),
        ],
        compiler_params=pltpu.CompilerParams(
            collective_id=0, has_side_effects=True, vmem_limit_bytes=50 * 2**20
        ),
    )(sb, id_rows, partial)
    flat = jnp.transpose(summed[:113].reshape(113, 6, 128), (1, 0, 2)).reshape(6, 113 * 128)
    remapped = flat[:, :14400].reshape(6, 64, 225)
    out_rows = to_chunk(jnp.transpose(remapped.reshape(6, 32, 2, 225), (1, 2, 0, 3)))
    rows = lax.all_to_all(out_rows, "col", 0, 0, tiled=True)
    back = pl.pallas_call(
        zonal_kernel,
        name="zonal",
        out_shape=jax.ShapeDtypeStruct((32, 24, 128), F32),
        in_specs=[vmem, vmem, vmem],
        out_specs=vmem,
        scratch_shapes=[pltpu.VMEM((2, 17, 64, 512), BF16)],
        compiler_params=pltpu.CompilerParams(vmem_limit_bytes=50 * 2**20),
    )(base_tables(), scales(cutoff), rows)
    filtered = from_chunk(lax.all_to_all(back, "col", 0, 0, tiled=True))
    filtered = jnp.transpose(filtered, (2, 0, 1, 3)).reshape(6, 64, 225)
    return remapped, filtered


def solution(mesh):
    in_specs = (
        P(None, ("band", "col")),
        P(("band", "col"), None, None),
        P(("band", "col")),
        P(("band", "col"), None),
        P(("band", "col")),
        P(("band", "col")),
    )
    out_specs = (P(None, "band", "col"), P(None, "band", "col"))
    return jax.shard_map(local, mesh=mesh, in_specs=in_specs, out_specs=out_specs, check_vma=False)
```

```python
import functools
import math

import jax
import jax.numpy as jnp
from jax import lax
from jax.experimental import pallas as pl
from jax.experimental.pallas import tpu as pltpu
from jax.sharding import PartitionSpec as P

NLON = 7200
KW = 512
CAP = 6
ROWS = 40
SENT = 37
TWO_PI = 6.283185307179586
MESH = pl.DeviceIdType.MESH
F32 = jnp.float32
BF16 = jnp.bfloat16
NZ, NX = 8, 4
GROUP = 32


def real_dft(xs):
    n = len(xs)
    if n == 1:
        return [(xs[0], None)]
    if n == 2:
        return [(xs[0] + xs[1], None), (xs[0] - xs[1], None)]
    even, odd = real_dft(xs[0::2]), real_dft(xs[1::2])
    half = n // 2

    def entry(spec, r):
        if r <= half // 2:
            re, im = spec[r]
            return re, im
        re, im = spec[half - r]
        return re, (None if im is None else -im)

    out = []
    for r in range(half + 1):
        if r == half:
            out.append((even[0][0] - odd[0][0], None))
            continue
        er, ei = entry(even, r)
        o_r, oi = entry(odd, r)
        if r == 0:
            out.append((er + o_r, None))
            continue
        if 4 * r == n:
            re = er if oi is None else er + oi
            im = -o_r if ei is None else ei - o_r
            out.append((re, im))
            continue
        c, s = math.cos(2 * math.pi * r / n), math.sin(2 * math.pi * r / n)
        if oi is None:
            tr, ti = c * o_r, -s * o_r
        else:
            tr, ti = c * o_r + s * oi, c * oi - s * o_r
        out.append((er + tr, ti if ei is None else ei + ti))
    return out


def real_idft(hs, n):
    if n == 1:
        return [hs[0][0]]
    if n == 2:
        return [hs[0][0] + hs[1][0], hs[0][0] - hs[1][0]]
    half = n // 2
    evens, odds = [], []
    for r in range(half // 2 + 1):
        re, im = hs[r]
        mr, mi = hs[half - r]
        sum_re, dif_re = re + mr, re - mr
        if r == 0:
            evens.append((sum_re, None))
            odds.append((dif_re, None))
            continue
        if 2 * r == half:
            evens.append((sum_re, None))
            odds.append((-2.0 * im, None))
            continue
        sum_im, dif_im = im - mi, im + mi
        c, s = math.cos(2 * math.pi * r / n), math.sin(2 * math.pi * r / n)
        evens.append((sum_re, sum_im))
        odds.append((c * dif_re - s * dif_im, c * dif_im + s * dif_re))
    a, b = real_idft(evens, half), real_idft(odds, half)
    out = []
    for x, y in zip(a, b):
        out += [x, y]
    return out


def halves(x):
    hi = x.astype(BF16)
    return hi, (x - hi.astype(F32)).astype(BF16)


def fill_tables(base_ref, table):
    ca, sa = base_ref[0:16, :], base_ref[16:32, :]
    for r in range(17):
        parts = []
        for k, sign in ((r, 1.0), (32 - r, -1.0)):
            cb = base_ref[32 + k : 33 + k, :]
            sb = base_ref[72 + k : 73 + k, :]
            c = ca * cb - sa * sb
            s = sa * cb + ca * sb
            parts.append((c, s, sign))
        for p, (c, s, sign) in enumerate(parts):
            for row, half, value in (
                (32 * p, 0, c),
                (32 * p, 1, sign * s),
                (32 * p + 16, 0, -s),
                (32 * p + 16, 1, sign * c),
            ):
                hi, lo = halves(value)
                table[0, r, row : row + 16, 256 * half : 256 * half + 256] = hi
                table[1, r, row : row + 16, 256 * half : 256 * half + 256] = lo


def scale_at(r, cut_ref):
    row = lax.broadcasted_iota(jnp.int32, (16, 64), 0)
    n = lax.broadcasted_iota(jnp.int32, (16, 64), 1)
    mirror = n >= 32
    k = 32 * (n & 15) + jnp.where(mirror, 32 - r, r)
    limit = jnp.where(row < 6, cut_ref[0], cut_ref[1])
    keep = k <= limit
    if r in (0, 16):
        keep = keep & (n < 32)
        weight = jnp.where(k > 0, 2.0 / NLON, 1.0 / NLON)
    else:
        weight = 1.0 / NLON
    return jnp.where(keep, weight, 0.0).astype(F32)


def zonal(rows_ref, out_ref, table, cut_ref):
    spec = real_dft([rows_ref[c] for c in range(32)])
    nt = (((1,), (1,)), ((), ()))
    nn = (((1,), (0,)), ((), ()))

    def widen(y):
        v0, v1, v2 = y[0:8], y[8:16], y[16:24]
        rolled = jnp.concatenate([v1[4:8], v1[0:4]], axis=0)
        return jnp.concatenate(
            [jnp.concatenate([v0, v1], axis=0), jnp.concatenate([v2, rolled], axis=0)], axis=1
        )

    def narrow(w):
        a, b = w[:, 0:128], w[:, 128:256]
        mid = jnp.concatenate([a[8:12], b[8:12]], axis=0)
        return jnp.concatenate([a[0:8], mid, b[0:8]], axis=0)

    back = []
    for r in range(17):
        re, im = spec[r]
        re = widen(re)
        im = jnp.zeros_like(re) if im is None else widen(im)
        hi, lo = halves(jnp.concatenate([re, im], axis=1))
        both = jnp.concatenate([hi, lo], axis=0)
        p = lax.dot_general(both, table[0, r], nt, preferred_element_type=F32)
        q = lax.dot_general(hi, table[1, r], nt, preferred_element_type=F32)
        s = (p[0:16] + p[16:32] + q) * scale_at(r, cut_ref)
        hi, lo = halves(s)
        both = jnp.concatenate([hi, lo], axis=0)
        p = lax.dot_general(both, table[0, r], nn, preferred_element_type=F32)
        q = lax.dot_general(hi, table[1, r], nn, preferred_element_type=F32)
        w = p[0:16] + p[16:32] + q
        back.append((narrow(w[:, 0:256]), None if r in (0, 16) else narrow(w[:, 256:512])))
    for c, value in enumerate(real_idft(back, 32)):
        out_ref[c] = value


def fill_base(base):
    for start, count, step in ((0, 16, 32), (32, 40, 1)):
        i = lax.broadcasted_iota(jnp.int32, (count, 256), 1)
        k = lax.broadcasted_iota(jnp.int32, (count, 256), 0) * step
        product = (i * k).astype(F32)
        turns = jnp.floor(product * (1.0 / NLON))
        phase = product - turns * NLON
        phase = jnp.where(phase < 0, phase + NLON, phase)
        phase = jnp.where(phase >= NLON, phase - NLON, phase)
        angle = phase * (TWO_PI / NLON)
        base[start : start + count, :] = jnp.where(i < 225, jnp.cos(angle), 0.0)
        base[start + count : start + 2 * count, :] = jnp.where(i < 225, jnp.sin(angle), 0.0)


def kernel(
    pick_ref, sb_ref, cut_ref, id_ref, src_ref, w_ref, remap_ref, filt_ref,
    wbuf, part, send, recv, data, tiles, flat, rtx, rrx, ztx, zrx, base, table,
    w_sem, send_sem, recv_sem, row_sem,
):
    bands = lax.axis_size("band")
    band, col = lax.axis_index("band"), lax.axis_index("col")
    z, x = col // NX, lax.rem(col, NX)
    cols = NZ * NX

    def weight_copy(g):
        return pltpu.make_async_copy(
            w_ref.at[pl.ds(g * GROUP, GROUP)], wbuf.at[pl.ds(g * GROUP, GROUP)], w_sem.at[g]
        )

    groups = wbuf.shape[0] // GROUP
    for g in range(groups):
        weight_copy(g).start()

    def peer(i):
        u, dx = i // NX, lax.rem(i, NX)
        m = (u + 1) // 2
        dz = jnp.where(lax.rem(u, 2) == 0, 4 + m, 4 - m)
        return lax.rem(z + dz, NZ) * NX + lax.rem(x + dx, NX)

    def targets(act):
        def step(i, carry):
            to = peer(i)
            for off in (0, 2, 1):
                other = band + off - 1
                if off == 1:
                    ok = to != col
                else:
                    ok = (other >= 0) & (other < bands)

                @pl.when(ok)
                def _(off=off, other=other):
                    act(off, other, to)

            return carry

        lax.fori_loop(0, cols, step, 0)

    barrier = pltpu.get_barrier_semaphore()
    targets(lambda off, b, c: pl.semaphore_signal(barrier, inc=1, device_id=(b, c), device_id_type=MESH))

    for side, edge in ((0, 0), (2, bands - 1)):

        @pl.when(band == edge)
        def _(side=side):
            recv[side] = jnp.full(recv.shape[1:], -1.0, F32)

    for g in range(groups):
        weight_copy(g).wait()

        def some(i, carry, g=g):
            first = g * GROUP + i * 8
            for n in range(8):
                k = first + n
                part[k] = jnp.dot(src_ref[pick_ref[k]], wbuf[k], preferred_element_type=F32)
            return carry

        lax.fori_loop(0, GROUP // 8, some, 0)

    def pack(j, carry):
        off, c = j // cols, lax.rem(j, cols)
        for s in range(CAP):
            send[off, c, pl.ds(s, 6, stride=CAP), :] = part[sb_ref[j * CAP + s]]
        send[off, c, 36:37, :] = id_ref[pl.ds(j, 1), :]
        return carry

    lax.fori_loop(0, 3 * cols, pack, 0)
    inner = (band > 0).astype(jnp.int32) + (band < bands - 1).astype(jnp.int32)
    pl.semaphore_wait(barrier, cols - 1 + cols * inner)

    def start(off, b, c):
        pltpu.make_async_remote_copy(
            src_ref=send.at[off, c, 0:SENT],
            dst_ref=recv.at[2 - off, col, 0:SENT],
            send_sem=send_sem.at[off],
            recv_sem=recv_sem.at[2 - off],
            device_id=(b, c),
            device_id_type=MESH,
        ).start()

    targets(start)
    pltpu.make_async_copy(send.at[1, col, 0:SENT], recv.at[1, col, 0:SENT], recv_sem.at[1]).start()
    data[...] = jnp.zeros_like(data)
    fill_base(base)
    fill_tables(base, table)

    def drain(off):
        pltpu.make_async_copy(recv.at[off, :, 0:SENT], recv.at[off, :, 0:SENT], recv_sem.at[off]).wait()

    def drain_send(off, n):
        pltpu.make_async_copy(
            send.at[off, 0:n, 0:SENT], send.at[off, 0:n, 0:SENT], send_sem.at[off]
        ).wait()

    drain(1)
    for off in (0, 2):
        other = band + off - 1

        @pl.when((other >= 0) & (other < bands))
        def _(off=off):
            drain(off)

    for off in range(3):

        def lay(c, carry, off=off):
            j = off * cols + c
            for lev in range(6):
                data[pl.ds(pl.multiple_of(j * 8, 8), 6), 128 * lev : 128 * lev + 128] = recv[
                    off, c, lev * CAP : lev * CAP + CAP, :
                ]
            return carry

        lax.fori_loop(0, cols, lay, 0)
    ids = recv[:, :, 36:37, :].reshape(3 * cols, 1, 128)
    lane = lax.broadcasted_iota(jnp.int32, (3 * cols, 8, 128), 2)
    sub = lax.broadcasted_iota(jnp.int32, (3 * cols, 8, 128), 1)
    diag = jnp.where(lane == sub, jnp.broadcast_to(ids, (3 * cols, 8, 128)), 0.0)
    diag = diag.reshape(24 * cols, 128).astype(BF16)
    spread = jnp.dot(diag, jnp.ones((128, 128), BF16), preferred_element_type=F32)
    tile = lax.broadcasted_iota(jnp.int32, (24 * cols, 128), 1).astype(F32)
    chooser = (spread == tile).astype(F32).astype(BF16)
    hi, lo = halves(data[...])
    tn = (((0,), (0,)), ((), ()))
    total = lax.dot_general(chooser, hi, tn, preferred_element_type=F32) + lax.dot_general(
        chooser, lo, tn, preferred_element_type=F32
    )
    for lev in range(6):
        tiles[pl.ds(lev, 128, stride=8), :] = total[:, 128 * lev : 128 * lev + 128]

    for lat in range(2 * cols):
        t, s = divmod(225 * lat, 128)
        a, b, c = (tiles[8 * (t + n) : 8 * (t + n) + 8, :] for n in range(3))
        if s:
            a, b, c = (pltpu.roll(v, 128 - s, 1) for v in (a, b, c))
            keep = lax.broadcasted_iota(jnp.int32, (8, 128), 1) < 128 - s
            a, b = jnp.where(keep, a, b), jnp.where(keep, b, c)
        a, b = a[0:6], b[0:6]
        flat[pl.ds(lat, 6, stride=64), :] = a
        flat[pl.ds(384 + lat, 6, stride=64), :] = b
        p = lat // 2
        if lat % 2 == 0:
            rtx[p, 0:6, :] = a
            rtx[p, 16:22, :] = b
        else:
            rtx[p, 6:12, :] = a
            rtx[p, 22:24, :] = b[0:2]
            rtx[p, 12:16, :] = b[2:6]

    def swap(src, dst, which):
        def step(i, carry):
            to = peer(i)

            @pl.when(to != col)
            def _():
                pltpu.make_async_remote_copy(
                    src_ref=src.at[to],
                    dst_ref=dst.at[col],
                    send_sem=row_sem.at[which, 0],
                    recv_sem=row_sem.at[which, 1],
                    device_id=(band, to),
                    device_id_type=MESH,
                ).start()

            return carry

        lax.fori_loop(0, cols, step, 0)
        pltpu.make_async_copy(src.at[col], dst.at[col], row_sem.at[which, 1]).start()

    def swapped(dst, which):
        pltpu.make_async_copy(dst, dst, row_sem.at[which, 1]).wait()

    def swap_sent(src, which):
        pltpu.make_async_copy(src.at[0 : cols - 1], src.at[0 : cols - 1], row_sem.at[which, 0]).wait()

    swap(rtx, rrx, 0)
    remap_ref[:, 0:128] = flat[0:384, :]
    remap_ref[:, 128:225] = flat[384:768, 0:97]
    drain_send(1, cols - 1)
    for off in (0, 2):
        other = band + off - 1

        @pl.when((other >= 0) & (other < bands))
        def _(off=off):
            drain_send(off, cols)

    swapped(rrx, 0)
    zonal(rrx, ztx, table, cut_ref)
    swap(ztx, zrx, 1)
    swap_sent(rtx, 0)
    swapped(zrx, 1)
    for lat in range(2 * cols):
        p = lat // 2
        if lat % 2 == 0:
            flat[pl.ds(lat, 6, stride=64), :] = zrx[p, 0:6, :]
            flat[pl.ds(384 + lat, 6, stride=64), :] = zrx[p, 16:22, :]
        else:
            flat[pl.ds(lat, 6, stride=64), :] = zrx[p, 6:12, :]
            flat[pl.ds(384 + lat, 2, stride=64), :] = zrx[p, 22:24, :]
            flat[pl.ds(512 + lat, 4, stride=64), :] = zrx[p, 12:16, :]
    filt_ref[:, 0:128] = flat[0:384, :]
    filt_ref[:, 128:225] = flat[384:768, 0:97]
    swap_sent(ztx, 1)


def local(source, weights, source_block, owner_device, target_tile, cutoff):
    cols = lax.axis_size("col")
    levels, nb, width = 6, weights.shape[0], weights.shape[1]
    band = lax.axis_index("band")
    blocks = jnp.transpose(source.reshape(levels, -1, width), (1, 0, 2))
    owners = owner_device[:, 0]
    row = lax.broadcasted_iota(jnp.int32, (nb, nb), 0)
    column = lax.broadcasted_iota(jnp.int32, (nb, nb), 1)
    earlier = (owners[None, :] == owners[:, None]) & (column < row)
    rank = jnp.sum(earlier.astype(jnp.int32), axis=1)
    slot = (owners - (band - 1) * cols) * CAP + rank
    total = 3 * cols * CAP
    hit = lax.broadcasted_iota(jnp.int32, (total, nb), 0) == slot[None, :]
    both = jnp.arange(nb, dtype=jnp.int32) * 128 + target_tile
    code = jnp.sum(jnp.where(hit, both[None, :] + 1, 0), axis=1)
    sb = jnp.maximum(code - 1, 0) // 128
    tid = jnp.where(code > 0, (code - 1) % 128, -1).astype(F32)
    id_rows = jnp.pad(tid.reshape(3 * cols, CAP), ((0, 0), (0, 128 - CAP)), constant_values=-1.0)
    vmem = pl.BlockSpec(memory_space=pltpu.VMEM)
    smem = pl.BlockSpec(memory_space=pltpu.SMEM)
    rows = (cols, 24, 128)
    remapped, filtered = pl.pallas_call(
        kernel,
        name="remap",
        out_shape=[jax.ShapeDtypeStruct((384, 225), F32)] * 2,
        in_specs=[smem, smem, smem, vmem, vmem, pl.BlockSpec(memory_space=pl.ANY)],
        out_specs=[vmem, vmem],
        scratch_shapes=[
            pltpu.VMEM((nb, width, width), BF16),
            pltpu.VMEM((nb, 6, 128), F32),
            pltpu.VMEM((3, cols, ROWS, 128), F32),
            pltpu.VMEM((3, cols, ROWS, 128), F32),
            pltpu.VMEM((24 * cols, 768), F32),
            pltpu.VMEM((1024, 128), F32),
            pltpu.VMEM((768, 128), F32),
            pltpu.VMEM(rows, F32),
            pltpu.VMEM(rows, F32),
            pltpu.VMEM(rows, F32),
            pltpu.VMEM(rows, F32),
            pltpu.VMEM((112, 256), F32),
            pltpu.VMEM((2, 17, 64, 512), BF16),
            pltpu.SemaphoreType.DMA((nb // GROUP,)),
            pltpu.SemaphoreType.DMA((3,)),
            pltpu.SemaphoreType.DMA((3,)),
            pltpu.SemaphoreType.DMA((2, 2)),
        ],
        compiler_params=pltpu.CompilerParams(
            collective_id=0, has_side_effects=True, vmem_limit_bytes=50 * 2**20
        ),
    )(source_block, sb, cutoff, id_rows, blocks, weights)
    return remapped.reshape(6, 64, 225), filtered.reshape(6, 64, 225)


def solution(mesh):
    in_specs = (
        P(None, ("band", "col")),
        P(("band", "col"), None, None),
        P(("band", "col")),
        P(("band", "col"), None),
        P(("band", "col")),
        P(("band", "col")),
    )
    out_specs = (P(None, "band", "col"), P(None, "band", "col"))
    return jax.shard_map(local, mesh=mesh, in_specs=in_specs, out_specs=out_specs, check_vma=False)
```

```python
import functools
import math

import jax
import jax.numpy as jnp
from jax import lax
from jax.experimental import pallas as pl
from jax.experimental.pallas import tpu as pltpu
from jax.sharding import PartitionSpec as P

NLON = 7200
KW = 512
CAP = 6
ROWS = 40
SENT = 37
TWO_PI = 6.283185307179586
MESH = pl.DeviceIdType.MESH
F32 = jnp.float32
BF16 = jnp.bfloat16
NZ, NX = 8, 4
GROUP = 32


def real_dft(xs):
    n = len(xs)
    if n == 1:
        return [(xs[0], None)]
    if n == 2:
        return [(xs[0] + xs[1], None), (xs[0] - xs[1], None)]
    even, odd = real_dft(xs[0::2]), real_dft(xs[1::2])
    half = n // 2

    def entry(spec, r):
        if r <= half // 2:
            re, im = spec[r]
            return re, im
        re, im = spec[half - r]
        return re, (None if im is None else -im)

    out = []
    for r in range(half + 1):
        if r == half:
            out.append((even[0][0] - odd[0][0], None))
            continue
        er, ei = entry(even, r)
        o_r, oi = entry(odd, r)
        if r == 0:
            out.append((er + o_r, None))
            continue
        if 4 * r == n:
            re = er if oi is None else er + oi
            im = -o_r if ei is None else ei - o_r
            out.append((re, im))
            continue
        c, s = math.cos(2 * math.pi * r / n), math.sin(2 * math.pi * r / n)
        if oi is None:
            tr, ti = c * o_r, -s * o_r
        else:
            tr, ti = c * o_r + s * oi, c * oi - s * o_r
        out.append((er + tr, ti if ei is None else ei + ti))
    return out


def real_idft(hs, n):
    if n == 1:
        return [hs[0][0]]
    if n == 2:
        return [hs[0][0] + hs[1][0], hs[0][0] - hs[1][0]]
    half = n // 2
    evens, odds = [], []
    for r in range(half // 2 + 1):
        re, im = hs[r]
        mr, mi = hs[half - r]
        sum_re, dif_re = re + mr, re - mr
        if r == 0:
            evens.append((sum_re, None))
            odds.append((dif_re, None))
            continue
        if 2 * r == half:
            evens.append((sum_re, None))
            odds.append((-2.0 * im, None))
            continue
        sum_im, dif_im = im - mi, im + mi
        c, s = math.cos(2 * math.pi * r / n), math.sin(2 * math.pi * r / n)
        evens.append((sum_re, sum_im))
        odds.append((c * dif_re - s * dif_im, c * dif_im + s * dif_re))
    a, b = real_idft(evens, half), real_idft(odds, half)
    out = []
    for x, y in zip(a, b):
        out += [x, y]
    return out


def halves(x):
    hi = x.astype(BF16)
    return hi, (x - hi.astype(F32)).astype(BF16)


def fill_tables(base_ref, table):
    ca, sa = base_ref[0:16, :], base_ref[16:32, :]
    for r in range(17):
        parts = []
        for k, sign in ((r, 1.0), (32 - r, -1.0)):
            cb = base_ref[32 + k : 33 + k, :]
            sb = base_ref[72 + k : 73 + k, :]
            c = ca * cb - sa * sb
            s = sa * cb + ca * sb
            parts.append((c, s, sign))
        for p, (c, s, sign) in enumerate(parts):
            for row, half, value in (
                (32 * p, 0, c),
                (32 * p, 1, sign * s),
                (32 * p + 16, 0, -s),
                (32 * p + 16, 1, sign * c),
            ):
                hi, lo = halves(value)
                table[0, r, row : row + 16, 256 * half : 256 * half + 256] = hi
                table[1, r, row : row + 16, 256 * half : 256 * half + 256] = lo


def scale_at(r, limit):
    n = lax.broadcasted_iota(jnp.int32, (8, 64), 1)
    mirror = n >= 32
    k = 32 * (n & 15) + jnp.where(mirror, 32 - r, r)
    keep = k <= limit
    if r in (0, 16):
        keep = keep & (n < 32)
        weight = jnp.where(k > 0, 2.0 / NLON, 1.0 / NLON)
    else:
        weight = 1.0 / NLON
    return jnp.where(keep, weight, 0.0).astype(F32)


def zonal(get, put, table, limit):
    spec = real_dft([get(c) for c in range(32)])
    nt = (((1,), (1,)), ((), ()))
    nn = (((1,), (0,)), ((), ()))

    def product(v, r, dims):
        hi, lo = halves(v)
        both = jnp.concatenate([hi, lo], axis=0)
        p = lax.dot_general(both, table[0, r], dims, preferred_element_type=F32)
        q = lax.dot_general(hi, table[1, r], dims, preferred_element_type=F32)
        return p[0:8] + p[8:16] + q

    back = []
    for r in range(17):
        re, im = spec[r]
        im = jnp.zeros_like(re) if im is None else im
        s = product(jnp.concatenate([re, im], axis=1), r, nt) * scale_at(r, limit)
        w = product(s, r, nn)
        back.append((w[:, 0:256], None if r in (0, 16) else w[:, 256:512]))
    for c, value in enumerate(real_idft(back, 32)):
        put(c, value)


def fill_base(base):
    for start, count, step in ((0, 16, 32), (32, 40, 1)):
        i = lax.broadcasted_iota(jnp.int32, (count, 256), 1)
        k = lax.broadcasted_iota(jnp.int32, (count, 256), 0) * step
        product = (i * k).astype(F32)
        turns = jnp.floor(product * (1.0 / NLON))
        phase = product - turns * NLON
        phase = jnp.where(phase < 0, phase + NLON, phase)
        phase = jnp.where(phase >= NLON, phase - NLON, phase)
        angle = phase * (TWO_PI / NLON)
        base[start : start + count, :] = jnp.where(i < 225, jnp.cos(angle), 0.0)
        base[start + count : start + 2 * count, :] = jnp.where(i < 225, jnp.sin(angle), 0.0)


def kernel(
    pick_ref, sb_ref, cut_ref, id_ref, src_ref, w_ref, remap_ref, filt_ref,
    wbuf, part, send, recv, data, own, dtx, drx, tiles, flat, rtx, rrx, ztx, zrx, base, table,
    w_sem, send_sem, recv_sem, dense_sem, row_sem,
):
    bands = lax.axis_size("band")
    band, col = lax.axis_index("band"), lax.axis_index("col")
    z, x = col // NX, lax.rem(col, NX)
    cols = NZ * NX
    planes = {0: (0, 1), 1: (1, 5), 2: (5, 8)}

    def weight_copy(g):
        return pltpu.make_async_copy(
            w_ref.at[pl.ds(g * GROUP, GROUP)], wbuf.at[pl.ds(g * GROUP, GROUP)], w_sem.at[g]
        )

    groups = wbuf.shape[0] // GROUP
    for g in range(groups):
        weight_copy(g).start()

    def valid(off):
        other = band + off - 1
        return (other >= 0) & (other < bands)

    barrier = pltpu.get_barrier_semaphore()

    def greet(c, carry):
        for off in (0, 1, 2):
            ok = c != col if off == 1 else valid(off)

            @pl.when(ok)
            def _(off=off):
                pl.semaphore_signal(barrier, inc=1, device_id=(band + off - 1, c), device_id_type=MESH)

        return carry

    lax.fori_loop(0, cols, greet, 0)

    for side, edge in ((0, 0), (2, bands - 1)):

        @pl.when(band == edge)
        def _(side=side):
            for d in range(NZ):
                first = d * 3 * NX + side * NX
                recv[first : first + NX] = jnp.full((NX, *recv.shape[1:]), -1.0, F32)

    for g in range(groups):
        weight_copy(g).wait()

        def some(i, carry, g=g):
            first = g * GROUP + i * 8
            for n in range(8):
                k = first + n
                part[k] = jnp.dot(src_ref[pick_ref[k]], wbuf[k], preferred_element_type=F32)
            return carry

        lax.fori_loop(0, GROUP // 8, some, 0)

    def turn(parity):
        return 1 - 2 * (parity & 1)

    def route(i, off):
        u = i // NX
        delta = jnp.where(u < 3, 5 + u, 7 - u)
        s = turn(band + off - 1)
        owner_z = lax.rem(z - s * delta + 2 * NZ, NZ)
        shift = jnp.where(delta == 0, 0, jnp.where(delta <= 4, s, -s))
        plane = lax.rem(owner_z + shift + NZ, NZ)
        to_x = lax.rem(x + i, NX)
        return owner_z * NX + to_x, delta, plane * NX + to_x

    def pack(i):
        for off in range(3):
            c, _, _ = route(i, off)
            j = off * cols + c
            for s in range(CAP):
                send[off, c, pl.ds(s, 6, stride=CAP), :] = part[sb_ref[j * CAP + s]]
            send[off, c, 36:37, :] = id_ref[pl.ds(j, 1), :]

    def transmit(i):
        for off in (0, 2, 1):
            c, delta, to = route(i, off)
            ok = to != col if off == 1 else valid(off)
            group = jnp.where(delta == 0, 0, jnp.where(delta <= 4, 1, 2))

            @pl.when(ok)
            def _(off=off, c=c, delta=delta, to=to, group=group):
                pltpu.make_async_remote_copy(
                    src_ref=send.at[off, c, 0:SENT],
                    dst_ref=recv.at[delta * 3 * NX + (2 - off) * NX + x, 0:SENT],
                    send_sem=send_sem.at[off],
                    recv_sem=recv_sem.at[group, 2 - off],
                    device_id=(band + off - 1, to),
                    device_id_type=MESH,
                ).start()

    pack(0)
    inner = (band > 0).astype(jnp.int32) + (band < bands - 1).astype(jnp.int32)
    pl.semaphore_wait(barrier, cols - 1 + cols * inner)

    def both(i, carry):
        @pl.when(i < cols - 1)
        def _():
            pack(i + 1)

        transmit(i)
        return carry

    lax.fori_loop(0, cols, both, 0)
    mine = turn(band)
    up = lax.rem(z + mine + NZ, NZ) * NX + x
    down = lax.rem(z - mine + NZ, NZ) * NX + x
    for c, delta, group in ((col, 0, 0), (down, 1, 1), (up, 7, 2)):
        pltpu.make_async_copy(
            send.at[1, c, 0:SENT],
            recv.at[delta * 3 * NX + NX + x, 0:SENT],
            recv_sem.at[group, 1],
        ).start()
    data[...] = jnp.zeros_like(data)
    fill_base(base)
    fill_tables(base, table)

    def take(group):
        first, last = planes[group]
        n = (last - first) * NX
        for off in range(3):
            wait = pltpu.make_async_copy(recv.at[0:n, 0:SENT], recv.at[0:n, 0:SENT], recv_sem.at[group, off])
            if off == 1:
                wait.wait()
            else:

                @pl.when(valid(off))
                def _(wait=wait):
                    wait.wait()

    def summed(group):
        first, last = (3 * NX * p for p in planes[group])
        n = last - first

        def lay(i, carry):
            j = first + i
            for lev in range(6):
                data[pl.ds(pl.multiple_of(j * 8, 8), 6), 128 * lev : 128 * lev + 128] = recv[
                    j, lev * CAP : lev * CAP + CAP, :
                ]
            return carry

        lax.fori_loop(0, n, lay, 0)
        ids = recv[first:last, 36:37, :].reshape(n, 1, 128)
        lane = lax.broadcasted_iota(jnp.int32, (n, 8, 128), 2)
        sub = lax.broadcasted_iota(jnp.int32, (n, 8, 128), 1)
        diag = jnp.where(lane == sub, jnp.broadcast_to(ids, (n, 8, 128)), 0.0)
        diag = diag.reshape(8 * n, 128).astype(BF16)
        spread = jnp.dot(diag, jnp.ones((128, 128), BF16), preferred_element_type=F32)
        tile = lax.broadcasted_iota(jnp.int32, (8 * n, 128), 1).astype(F32)
        chooser = (spread == tile).astype(F32).astype(BF16)
        hi, lo = halves(data[8 * first : 8 * last, :])
        tn = (((0,), (0,)), ((), ()))
        return lax.dot_general(chooser, hi, tn, preferred_element_type=F32) + lax.dot_general(
            chooser, lo, tn, preferred_element_type=F32
        )

    def dense(which, to):
        return pltpu.make_async_remote_copy(
            src_ref=dtx.at[which, :, 0:113],
            dst_ref=drx.at[which, :, 0:113],
            send_sem=dense_sem.at[which, 0],
            recv_sem=dense_sem.at[which, 1],
            device_id=(band, to),
            device_id_type=MESH,
        )

    for group, which, to in ((2, 1, up), (0, None, None), (1, 0, down)):
        take(group)
        total = summed(group)
        if which is None:
            own[...] = total
            continue
        for lev in range(6):
            dtx[which, lev] = total[0:120, 128 * lev : 128 * lev + 128]
        dense(which, to).start()

    dense(1, up).wait()
    dense(0, down).wait()
    for lev in range(6):
        tiles[pl.ds(lev, 120, stride=8), :] = (
            own[0:120, 128 * lev : 128 * lev + 128] + drx[0, lev] + drx[1, lev]
        )

    def row(lat):
        t, s = divmod(225 * lat, 128)
        a, b, c = (tiles[8 * (t + n) : 8 * (t + n) + 8, :] for n in range(3))
        if s:
            a, b, c = (pltpu.roll(v, 128 - s, 1) for v in (a, b, c))
            keep = lax.broadcasted_iota(jnp.int32, (8, 128), 1) < 128 - s
            a, b = jnp.where(keep, a, b), jnp.where(keep, b, c)
        return a[0:6], b[0:6]

    def swap(src, dst, which, j):
        def step(i, carry):
            u = i // NX
            m = (u + 1) // 2
            dz = jnp.where(lax.rem(u, 2) == 0, 4 + m, 4 - m)
            to = lax.rem(z + dz, NZ) * NX + lax.rem(x + i, NX)

            @pl.when(to != col)
            def _():
                pltpu.make_async_remote_copy(
                    src_ref=src.at[j, to, 0:12],
                    dst_ref=dst.at[j, col, 0:12],
                    send_sem=row_sem.at[which, j, 0],
                    recv_sem=row_sem.at[which, j, 1],
                    device_id=(band, to),
                    device_id_type=MESH,
                ).start()

            return carry

        lax.fori_loop(0, cols, step, 0)
        pltpu.make_async_copy(src.at[j, col, 0:12], dst.at[j, col, 0:12], row_sem.at[which, j, 1]).start()

    def swapped(dst, which, j):
        pltpu.make_async_copy(dst.at[j, :, 0:12], dst.at[j, :, 0:12], row_sem.at[which, j, 1]).wait()

    def swap_sent(src, which, j):
        part_of = src.at[j, 0 : cols - 1, 0:12]
        pltpu.make_async_copy(part_of, part_of, row_sem.at[which, j, 0]).wait()

    for j in range(2):
        for lat in range(j, 2 * cols, 2):
            a, b = row(lat)
            flat[pl.ds(lat, 6, stride=64), :] = a
            flat[pl.ds(384 + lat, 6, stride=64), :] = b
            rtx[j, lat // 2, 0:6, :] = a
            rtx[j, lat // 2, 6:12, :] = b
        swap(rtx, rrx, 0, j)
    remap_ref[:, 0:128] = flat[0:384, :]
    remap_ref[:, 128:225] = flat[384:768, 0:97]

    for j in range(2):
        swapped(rrx, 0, j)

        def get(c, j=j):
            return jnp.concatenate([rrx[j, c, 0:8, :], rrx[j, c, 6:14, :]], axis=1)

        def put(c, value, j=j):
            ztx[j, c, 0:6, :] = value[0:6, 0:128]
            ztx[j, c, 6:12, :] = value[0:6, 128:256]

        zonal(get, put, table, cut_ref[j])
        swap(ztx, zrx, 1, j)

    pltpu.make_async_copy(
        send.at[1, 0 : cols - 3, 0:SENT], send.at[1, 0 : cols - 3, 0:SENT], send_sem.at[1]
    ).wait()
    for off in (0, 2):

        @pl.when(valid(off))
        def _(off=off):
            pltpu.make_async_copy(send.at[off, :, 0:SENT], send.at[off, :, 0:SENT], send_sem.at[off]).wait()

    for j in range(2):
        swap_sent(rtx, 0, j)
    for j in range(2):
        swapped(zrx, 1, j)
        for lat in range(j, 2 * cols, 2):
            flat[pl.ds(lat, 6, stride=64), :] = zrx[j, lat // 2, 0:6, :]
            flat[pl.ds(384 + lat, 6, stride=64), :] = zrx[j, lat // 2, 6:12, :]
    filt_ref[:, 0:128] = flat[0:384, :]
    filt_ref[:, 128:225] = flat[384:768, 0:97]
    for j in range(2):
        swap_sent(ztx, 1, j)


def local(source, weights, source_block, owner_device, target_tile, cutoff):
    cols = lax.axis_size("col")
    levels, nb, width = 6, weights.shape[0], weights.shape[1]
    band = lax.axis_index("band")
    blocks = jnp.transpose(source.reshape(levels, -1, width), (1, 0, 2))
    owners = owner_device[:, 0]
    row = lax.broadcasted_iota(jnp.int32, (nb, nb), 0)
    column = lax.broadcasted_iota(jnp.int32, (nb, nb), 1)
    earlier = (owners[None, :] == owners[:, None]) & (column < row)
    rank = jnp.sum(earlier.astype(jnp.int32), axis=1)
    slot = (owners - (band - 1) * cols) * CAP + rank
    total = 3 * cols * CAP
    hit = lax.broadcasted_iota(jnp.int32, (total, nb), 0) == slot[None, :]
    both = jnp.arange(nb, dtype=jnp.int32) * 128 + target_tile
    code = jnp.sum(jnp.where(hit, both[None, :] + 1, 0), axis=1)
    sb = jnp.maximum(code - 1, 0) // 128
    tid = jnp.where(code > 0, (code - 1) % 128, -1).astype(F32)
    id_rows = jnp.pad(tid.reshape(3 * cols, CAP), ((0, 0), (0, 128 - CAP)), constant_values=-1.0)
    vmem = pl.BlockSpec(memory_space=pltpu.VMEM)
    smem = pl.BlockSpec(memory_space=pltpu.SMEM)
    rows = (2, cols, 16, 128)
    remapped, filtered = pl.pallas_call(
        kernel,
        name="remap",
        out_shape=[jax.ShapeDtypeStruct((384, 225), F32)] * 2,
        in_specs=[smem, smem, smem, vmem, vmem, pl.BlockSpec(memory_space=pl.ANY)],
        out_specs=[vmem, vmem],
        scratch_shapes=[
            pltpu.VMEM((nb, width, width), BF16),
            pltpu.VMEM((nb, 6, 128), F32),
            pltpu.VMEM((3, cols, ROWS, 128), F32),
            pltpu.VMEM((3 * cols, ROWS, 128), F32),
            pltpu.VMEM((24 * cols, 768), F32),
            pltpu.VMEM((128, 768), F32),
            pltpu.VMEM((2, 6, 120, 128), F32),
            pltpu.VMEM((2, 6, 120, 128), F32),
            pltpu.VMEM((1024, 128), F32),
            pltpu.VMEM((768, 128), F32),
            pltpu.VMEM(rows, F32),
            pltpu.VMEM(rows, F32),
            pltpu.VMEM(rows, F32),
            pltpu.VMEM(rows, F32),
            pltpu.VMEM((112, 256), F32),
            pltpu.VMEM((2, 17, 64, 512), BF16),
            pltpu.SemaphoreType.DMA((nb // GROUP,)),
            pltpu.SemaphoreType.DMA((3,)),
            pltpu.SemaphoreType.DMA((3, 3)),
            pltpu.SemaphoreType.DMA((2, 2)),
            pltpu.SemaphoreType.DMA((2, 2, 2)),
        ],
        compiler_params=pltpu.CompilerParams(
            collective_id=0, has_side_effects=True, vmem_limit_bytes=50 * 2**20
        ),
    )(source_block, sb, cutoff, id_rows, blocks, weights)
    return remapped.reshape(6, 64, 225), filtered.reshape(6, 64, 225)


def solution(mesh):
    in_specs = (
        P(None, ("band", "col")),
        P(("band", "col"), None, None),
        P(("band", "col")),
        P(("band", "col"), None),
        P(("band", "col")),
        P(("band", "col")),
    )
    out_specs = (P(None, "band", "col"), P(None, "band", "col"))
    return jax.shard_map(local, mesh=mesh, in_specs=in_specs, out_specs=out_specs, check_vma=False)
```

```python
import functools
import math

import jax
import jax.numpy as jnp
from jax import lax
from jax.experimental import pallas as pl
from jax.experimental.pallas import tpu as pltpu
from jax.sharding import PartitionSpec as P

NLON = 7200
KW = 512
CAP = 6
ROWS = 40
SENT = 37
TWO_PI = 6.283185307179586
MESH = pl.DeviceIdType.MESH
F32 = jnp.float32
BF16 = jnp.bfloat16
NZ, NX = 8, 4
GROUP = 32


def real_dft(xs):
    n = len(xs)
    if n == 1:
        return [(xs[0], None)]
    if n == 2:
        return [(xs[0] + xs[1], None), (xs[0] - xs[1], None)]
    even, odd = real_dft(xs[0::2]), real_dft(xs[1::2])
    half = n // 2

    def entry(spec, r):
        if r <= half // 2:
            re, im = spec[r]
            return re, im
        re, im = spec[half - r]
        return re, (None if im is None else -im)

    out = []
    for r in range(half + 1):
        if r == half:
            out.append((even[0][0] - odd[0][0], None))
            continue
        er, ei = entry(even, r)
        o_r, oi = entry(odd, r)
        if r == 0:
            out.append((er + o_r, None))
            continue
        if 4 * r == n:
            re = er if oi is None else er + oi
            im = -o_r if ei is None else ei - o_r
            out.append((re, im))
            continue
        c, s = math.cos(2 * math.pi * r / n), math.sin(2 * math.pi * r / n)
        if oi is None:
            tr, ti = c * o_r, -s * o_r
        else:
            tr, ti = c * o_r + s * oi, c * oi - s * o_r
        out.append((er + tr, ti if ei is None else ei + ti))
    return out


def real_idft(hs, n):
    if n == 1:
        return [hs[0][0]]
    if n == 2:
        return [hs[0][0] + hs[1][0], hs[0][0] - hs[1][0]]
    half = n // 2
    evens, odds = [], []
    for r in range(half // 2 + 1):
        re, im = hs[r]
        mr, mi = hs[half - r]
        sum_re, dif_re = re + mr, re - mr
        if r == 0:
            evens.append((sum_re, None))
            odds.append((dif_re, None))
            continue
        if 2 * r == half:
            evens.append((sum_re, None))
            odds.append((-2.0 * im, None))
            continue
        sum_im, dif_im = im - mi, im + mi
        c, s = math.cos(2 * math.pi * r / n), math.sin(2 * math.pi * r / n)
        evens.append((sum_re, sum_im))
        odds.append((c * dif_re - s * dif_im, c * dif_im + s * dif_re))
    a, b = real_idft(evens, half), real_idft(odds, half)
    out = []
    for x, y in zip(a, b):
        out += [x, y]
    return out


def halves(x):
    hi = x.astype(BF16)
    return hi, (x - hi.astype(F32)).astype(BF16)


def fill_tables(base_ref, table):
    ca, sa = base_ref[0:16, :], base_ref[16:32, :]
    for r in range(17):
        parts = []
        for k, sign in ((r, 1.0), (32 - r, -1.0)):
            cb = base_ref[32 + k : 33 + k, :]
            sb = base_ref[72 + k : 73 + k, :]
            c = ca * cb - sa * sb
            s = sa * cb + ca * sb
            parts.append((c, s, sign))
        for p, (c, s, sign) in enumerate(parts):
            for row, half, value in (
                (32 * p, 0, c),
                (32 * p, 1, sign * s),
                (32 * p + 16, 0, -s),
                (32 * p + 16, 1, sign * c),
            ):
                hi, lo = halves(value)
                table[0, r, row : row + 16, 256 * half : 256 * half + 256] = hi
                table[1, r, row : row + 16, 256 * half : 256 * half + 256] = lo


def scale_at(r, limit):
    n = lax.broadcasted_iota(jnp.int32, (8, 64), 1)
    mirror = n >= 32
    k = 32 * (n & 15) + jnp.where(mirror, 32 - r, r)
    keep = k <= limit
    if r in (0, 16):
        keep = keep & (n < 32)
        weight = jnp.where(k > 0, 2.0 / NLON, 1.0 / NLON)
    else:
        weight = 1.0 / NLON
    return jnp.where(keep, weight, 0.0).astype(F32)


def zonal(get, put, table, limit):
    spec = real_dft([get(c) for c in range(32)])
    nt = (((1,), (1,)), ((), ()))
    nn = (((1,), (0,)), ((), ()))

    def product(v, r, dims):
        hi, lo = halves(v)
        both = jnp.concatenate([hi, lo], axis=0)
        p = lax.dot_general(both, table[0, r], dims, preferred_element_type=F32)
        q = lax.dot_general(hi, table[1, r], dims, preferred_element_type=F32)
        return p[0:8] + p[8:16] + q

    back = []
    for r in range(17):
        re, im = spec[r]
        im = jnp.zeros_like(re) if im is None else im
        s = product(jnp.concatenate([re, im], axis=1), r, nt) * scale_at(r, limit)
        w = product(s, r, nn)
        back.append((w[:, 0:256], None if r in (0, 16) else w[:, 256:512]))
    for c, value in enumerate(real_idft(back, 32)):
        put(c, value)


def fill_base(base):
    for start, count, step in ((0, 16, 32), (32, 40, 1)):
        i = lax.broadcasted_iota(jnp.int32, (count, 256), 1)
        k = lax.broadcasted_iota(jnp.int32, (count, 256), 0) * step
        product = (i * k).astype(F32)
        turns = jnp.floor(product * (1.0 / NLON))
        phase = product - turns * NLON
        phase = jnp.where(phase < 0, phase + NLON, phase)
        phase = jnp.where(phase >= NLON, phase - NLON, phase)
        angle = phase * (TWO_PI / NLON)
        base[start : start + count, :] = jnp.where(i < 225, jnp.cos(angle), 0.0)
        base[start + count : start + 2 * count, :] = jnp.where(i < 225, jnp.sin(angle), 0.0)


def slot_table(meta_ref, band, cols, slot_ref, id_ref):
    nt = (((1,), (1,)), ((), ()))
    nb = meta_ref.shape[1]
    owner = meta_ref[0:1, :] - (band - 1) * cols
    sub = lax.broadcasted_iota(jnp.int32, (nb, nb), 0)
    lane = lax.broadcasted_iota(jnp.int32, (nb, nb), 1)
    across = jnp.broadcast_to(owner, (nb, nb))
    down = jnp.transpose(across)
    earlier = jnp.where((down == across) & (sub < lane), 1, 0)
    rank = jnp.sum(earlier, axis=0, keepdims=True)
    rank_down = jnp.transpose(jnp.broadcast_to(rank, (128, nb)))
    near = down[:, 0:128] == lane[:, 0:128]
    for s in range(CAP):
        here = jnp.where(near & (rank_down == s), sub[:, 0:128], 0)
        slot_ref[s : s + 1, :] = jnp.sum(here, axis=0, keepdims=True)
    number = lax.broadcasted_iota(jnp.int32, (128, nb), 0)
    to = (jnp.broadcast_to(owner, (128, nb)) == number).astype(F32).astype(BF16)
    tile = (meta_ref[1:2, :] + 1).astype(F32)
    tiles = jnp.where(jnp.broadcast_to(rank, (128, nb)) == number, tile, 0.0).astype(BF16)
    id_ref[...] = lax.dot_general(to, tiles, nt, preferred_element_type=F32) - 1.0


def kernel(
    meta_ref, src_ref, w_ref, remap_ref, filt_ref,
    pick_ref, slot_ref, sb_ref, id_ref, wbuf, part, send, recv, data, own, dtx, drx, tiles, flat, rtx, rrx, ztx, zrx, base, table,
    in_sem, w_sem, send_sem, recv_sem, dense_sem, row_sem, pair_sem,
):
    bands = lax.axis_size("band")
    band, col = lax.axis_index("band"), lax.axis_index("col")
    z, x = col // NX, lax.rem(col, NX)
    cols = NZ * NX
    planes = {0: (0, 1), 1: (1, 5), 2: (5, 8)}

    pick_copy = pltpu.make_async_copy(meta_ref.at[2:4], pick_ref, in_sem.at[0])
    pick_copy.start()

    def weight_copy(g):
        return pltpu.make_async_copy(
            w_ref.at[pl.ds(g * GROUP, GROUP)], wbuf.at[pl.ds(g * GROUP, GROUP)], w_sem.at[g]
        )

    groups = wbuf.shape[0] // GROUP
    for g in range(groups):
        weight_copy(g).start()

    def valid(off):
        other = band + off - 1
        return (other >= 0) & (other < bands)

    barrier = pltpu.get_barrier_semaphore()

    def greet(c, carry):
        for off in (0, 1, 2):
            ok = c != col if off == 1 else valid(off)

            @pl.when(ok)
            def _(off=off):
                pl.semaphore_signal(barrier, inc=1, device_id=(band + off - 1, c), device_id_type=MESH)

        return carry

    lax.fori_loop(0, cols, greet, 0)

    for side, edge in ((0, 0), (2, bands - 1)):

        @pl.when(band == edge)
        def _(side=side):
            for d in range(NZ):
                first = d * 3 * NX + side * NX
                recv[first : first + NX] = jnp.full((NX, *recv.shape[1:]), -1.0, F32)

    pick_copy.wait()
    table_copy = pltpu.make_async_copy(slot_ref, sb_ref, in_sem.at[1])

    for g in range(groups):
        weight_copy(g).wait()

        def some(i, carry, g=g):
            first = g * GROUP + i * 8
            for n in range(8):
                k = first + n
                part[k] = jnp.dot(src_ref[pick_ref[0, k]], wbuf[k], preferred_element_type=F32)
            return carry

        lax.fori_loop(0, GROUP // 8, some, 0)
        if g == 0:
            slot_table(meta_ref, band, cols, slot_ref, id_ref)
            table_copy.start()

    def turn(parity):
        return 1 - 2 * (parity & 1)

    def route(i, off):
        u = i // NX
        delta = jnp.where(u < 3, 5 + u, 7 - u)
        s = turn(band + off - 1)
        owner_z = lax.rem(z - s * delta + 2 * NZ, NZ)
        shift = jnp.where(delta == 0, 0, jnp.where(delta <= 4, s, -s))
        plane = lax.rem(owner_z + shift + NZ, NZ)
        to_x = lax.rem(x + i, NX)
        return owner_z * NX + to_x, delta, plane * NX + to_x

    def pack(i):
        for off in range(3):
            c, _, _ = route(i, off)
            j = off * cols + c
            for s in range(CAP):
                send[off, c, pl.ds(s, 6, stride=CAP), :] = part[sb_ref[s, j]]
            send[off, c, 36:37, :] = id_ref[pl.ds(j, 1), :]

    def transmit(i):
        for off in (0, 2, 1):
            c, delta, to = route(i, off)
            ok = to != col if off == 1 else valid(off)
            group = jnp.where(delta == 0, 0, jnp.where(delta <= 4, 1, 2))

            @pl.when(ok)
            def _(off=off, c=c, delta=delta, to=to, group=group):
                pltpu.make_async_remote_copy(
                    src_ref=send.at[off, c, 0:SENT],
                    dst_ref=recv.at[delta * 3 * NX + (2 - off) * NX + x, 0:SENT],
                    send_sem=send_sem.at[off],
                    recv_sem=recv_sem.at[group, 2 - off],
                    device_id=(band + off - 1, to),
                    device_id_type=MESH,
                ).start()

    table_copy.wait()
    pack(0)
    inner = (band > 0).astype(jnp.int32) + (band < bands - 1).astype(jnp.int32)
    pl.semaphore_wait(barrier, cols - 1 + cols * inner)

    def both(i, carry):
        @pl.when(i < cols - 1)
        def _():
            pack(i + 1)

        transmit(i)
        return carry

    lax.fori_loop(0, cols, both, 0)
    mine = turn(band)
    up = lax.rem(z + mine + NZ, NZ) * NX + x
    down = lax.rem(z - mine + NZ, NZ) * NX + x
    for c, delta, group in ((col, 0, 0), (down, 1, 1), (up, 7, 2)):
        pltpu.make_async_copy(
            send.at[1, c, 0:SENT],
            recv.at[delta * 3 * NX + NX + x, 0:SENT],
            recv_sem.at[group, 1],
        ).start()
    data[...] = jnp.zeros_like(data)
    fill_base(base)
    fill_tables(base, table)

    def take(group):
        first, last = planes[group]
        n = (last - first) * NX
        for off in range(3):
            wait = pltpu.make_async_copy(recv.at[0:n, 0:SENT], recv.at[0:n, 0:SENT], recv_sem.at[group, off])
            if off == 1:
                wait.wait()
            else:

                @pl.when(valid(off))
                def _(wait=wait):
                    wait.wait()

    def summed(group):
        first, last = (3 * NX * p for p in planes[group])
        n = last - first

        def lay(i, carry):
            j = first + i
            for lev in range(6):
                data[pl.ds(pl.multiple_of(j * 8, 8), 6), 128 * lev : 128 * lev + 128] = recv[
                    j, lev * CAP : lev * CAP + CAP, :
                ]
            return carry

        lax.fori_loop(0, n, lay, 0)
        ids = recv[first:last, 36:37, :].reshape(n, 1, 128)
        lane = lax.broadcasted_iota(jnp.int32, (n, 8, 128), 2)
        sub = lax.broadcasted_iota(jnp.int32, (n, 8, 128), 1)
        diag = jnp.where(lane == sub, jnp.broadcast_to(ids, (n, 8, 128)), 0.0)
        diag = diag.reshape(8 * n, 128).astype(BF16)
        spread = jnp.dot(diag, jnp.ones((128, 128), BF16), preferred_element_type=F32)
        tile = lax.broadcasted_iota(jnp.int32, (8 * n, 128), 1).astype(F32)
        chooser = (spread == tile).astype(F32).astype(BF16)
        hi, lo = halves(data[8 * first : 8 * last, :])
        tn = (((0,), (0,)), ((), ()))
        return lax.dot_general(chooser, hi, tn, preferred_element_type=F32) + lax.dot_general(
            chooser, lo, tn, preferred_element_type=F32
        )

    def dense(which, to):
        return pltpu.make_async_remote_copy(
            src_ref=dtx.at[which, :, 0:113],
            dst_ref=drx.at[which, :, 0:113],
            send_sem=dense_sem.at[which, 0],
            recv_sem=dense_sem.at[which, 1],
            device_id=(band, to),
            device_id_type=MESH,
        )

    for group, which, to in ((2, 1, up), (0, None, None), (1, 0, down)):
        take(group)
        total = summed(group)
        if which is None:
            own[...] = total
            continue
        for lev in range(6):
            dtx[which, lev] = total[0:120, 128 * lev : 128 * lev + 128]
        dense(which, to).start()

    dense(1, up).wait()
    dense(0, down).wait()
    for lev in range(6):
        tiles[pl.ds(lev, 120, stride=8), :] = (
            own[0:120, 128 * lev : 128 * lev + 128] + drx[0, lev] + drx[1, lev]
        )

    pl.semaphore_signal(pair_sem, inc=1, device_id=(band + turn(band), col), device_id_type=MESH)
    pl.semaphore_wait(pair_sem, 1)

    def row(lat):
        t, s = divmod(225 * lat, 128)
        a, b, c = (tiles[8 * (t + n) : 8 * (t + n) + 8, :] for n in range(3))
        if s:
            a, b, c = (pltpu.roll(v, 128 - s, 1) for v in (a, b, c))
            keep = lax.broadcasted_iota(jnp.int32, (8, 128), 1) < 128 - s
            a, b = jnp.where(keep, a, b), jnp.where(keep, b, c)
        return a[0:6], b[0:6]

    def swap(src, dst, which, j):
        def step(i, carry):
            u = i // NX
            m = (u + 1) // 2
            dz = jnp.where(lax.rem(u, 2) == 0, 4 + m, 4 - m)
            to = lax.rem(z + dz, NZ) * NX + lax.rem(x + i, NX)

            @pl.when(to != col)
            def _():
                pltpu.make_async_remote_copy(
                    src_ref=src.at[j, to, 0:12],
                    dst_ref=dst.at[j, col, 0:12],
                    send_sem=row_sem.at[which, j, 0],
                    recv_sem=row_sem.at[which, j, 1],
                    device_id=(band, to),
                    device_id_type=MESH,
                ).start()

            return carry

        lax.fori_loop(0, cols, step, 0)
        pltpu.make_async_copy(src.at[j, col, 0:12], dst.at[j, col, 0:12], row_sem.at[which, j, 1]).start()

    def swapped(dst, which, j):
        pltpu.make_async_copy(dst.at[j, :, 0:12], dst.at[j, :, 0:12], row_sem.at[which, j, 1]).wait()

    def swap_sent(src, which, j):
        part_of = src.at[j, 0 : cols - 1, 0:12]
        pltpu.make_async_copy(part_of, part_of, row_sem.at[which, j, 0]).wait()

    for j in range(2):
        for lat in range(j, 2 * cols, 2):
            a, b = row(lat)
            flat[pl.ds(lat, 6, stride=64), :] = a
            flat[pl.ds(384 + lat, 6, stride=64), :] = b
            rtx[j, lat // 2, 0:6, :] = a
            rtx[j, lat // 2, 6:12, :] = b
        swap(rtx, rrx, 0, j)
    remap_ref[:, 0:128] = flat[0:384, :]
    remap_ref[:, 128:225] = flat[384:768, 0:97]

    for j in range(2):
        swapped(rrx, 0, j)

        def get(c, j=j):
            return jnp.concatenate([rrx[j, c, 0:8, :], rrx[j, c, 6:14, :]], axis=1)

        def put(c, value, j=j):
            ztx[j, c, 0:6, :] = value[0:6, 0:128]
            ztx[j, c, 6:12, :] = value[0:6, 128:256]

        zonal(get, put, table, pick_ref[1, j])
        swap(ztx, zrx, 1, j)

    pltpu.make_async_copy(
        send.at[1, 0 : cols - 3, 0:SENT], send.at[1, 0 : cols - 3, 0:SENT], send_sem.at[1]
    ).wait()
    for off in (0, 2):

        @pl.when(valid(off))
        def _(off=off):
            pltpu.make_async_copy(send.at[off, :, 0:SENT], send.at[off, :, 0:SENT], send_sem.at[off]).wait()

    for j in range(2):
        swap_sent(rtx, 0, j)
    for j in range(2):
        swapped(zrx, 1, j)
        for lat in range(j, 2 * cols, 2):
            flat[pl.ds(lat, 6, stride=64), :] = zrx[j, lat // 2, 0:6, :]
            flat[pl.ds(384 + lat, 6, stride=64), :] = zrx[j, lat // 2, 6:12, :]
    filt_ref[:, 0:128] = flat[0:384, :]
    filt_ref[:, 128:225] = flat[384:768, 0:97]
    for j in range(2):
        swap_sent(ztx, 1, j)


def local(source, weights, source_block, owner_device, target_tile, cutoff):
    cols = lax.axis_size("col")
    levels, nb, width = 6, weights.shape[0], weights.shape[1]
    blocks = jnp.transpose(source.reshape(levels, -1, width), (1, 0, 2))
    limit = jnp.pad(cutoff, (0, nb - cutoff.shape[0]))
    meta = jnp.stack([owner_device[:, 0], target_tile, source_block, limit])
    vmem = pl.BlockSpec(memory_space=pltpu.VMEM)
    rows = (2, cols, 16, 128)
    remapped, filtered = pl.pallas_call(
        kernel,
        name="remap",
        out_shape=[jax.ShapeDtypeStruct((384, 225), F32)] * 2,
        in_specs=[vmem, vmem, pl.BlockSpec(memory_space=pl.ANY)],
        out_specs=[vmem, vmem],
        scratch_shapes=[
            pltpu.SMEM((2, nb), jnp.int32),
            pltpu.VMEM((8, 128), jnp.int32),
            pltpu.SMEM((8, 128), jnp.int32),
            pltpu.VMEM((128, 128), F32),
            pltpu.VMEM((nb, width, width), BF16),
            pltpu.VMEM((nb, 6, 128), F32),
            pltpu.VMEM((3, cols, ROWS, 128), F32),
            pltpu.VMEM((3 * cols, ROWS, 128), F32),
            pltpu.VMEM((24 * cols, 768), F32),
            pltpu.VMEM((128, 768), F32),
            pltpu.VMEM((2, 6, 120, 128), F32),
            pltpu.VMEM((2, 6, 120, 128), F32),
            pltpu.VMEM((1024, 128), F32),
            pltpu.VMEM((768, 128), F32),
            pltpu.VMEM(rows, F32),
            pltpu.VMEM(rows, F32),
            pltpu.VMEM(rows, F32),
            pltpu.VMEM(rows, F32),
            pltpu.VMEM((112, 256), F32),
            pltpu.VMEM((2, 17, 64, 512), BF16),
            pltpu.SemaphoreType.DMA((2,)),
            pltpu.SemaphoreType.DMA((nb // GROUP,)),
            pltpu.SemaphoreType.DMA((3,)),
            pltpu.SemaphoreType.DMA((3, 3)),
            pltpu.SemaphoreType.DMA((2, 2)),
            pltpu.SemaphoreType.DMA((2, 2, 2)),
            pltpu.SemaphoreType.REGULAR,
        ],
        compiler_params=pltpu.CompilerParams(
            collective_id=0, has_side_effects=True, vmem_limit_bytes=50 * 2**20
        ),
    )(meta, blocks, weights)
    return remapped.reshape(6, 64, 225), filtered.reshape(6, 64, 225)


def solution(mesh):
    in_specs = (
        P(None, ("band", "col")),
        P(("band", "col"), None, None),
        P(("band", "col")),
        P(("band", "col"), None),
        P(("band", "col")),
        P(("band", "col")),
    )
    out_specs = (P(None, "band", "col"), P(None, "band", "col"))
    return jax.shard_map(local, mesh=mesh, in_specs=in_specs, out_specs=out_specs, check_vma=False)
```

```python
import functools
import math

import jax
import jax.numpy as jnp
from jax import lax
from jax.experimental import pallas as pl
from jax.experimental.pallas import tpu as pltpu
from jax.sharding import PartitionSpec as P

NLON = 7200
KW = 512
CAP = 6
ROWS = 40
SENT = 37
TWO_PI = 6.283185307179586
MESH = pl.DeviceIdType.MESH
F32 = jnp.float32
BF16 = jnp.bfloat16
NZ, NX = 8, 4
GROUP = 32


def real_dft(xs):
    n = len(xs)
    if n == 1:
        return [(xs[0], None)]
    if n == 2:
        return [(xs[0] + xs[1], None), (xs[0] - xs[1], None)]
    even, odd = real_dft(xs[0::2]), real_dft(xs[1::2])
    half = n // 2

    def entry(spec, r):
        if r <= half // 2:
            re, im = spec[r]
            return re, im
        re, im = spec[half - r]
        return re, (None if im is None else -im)

    out = []
    for r in range(half + 1):
        if r == half:
            out.append((even[0][0] - odd[0][0], None))
            continue
        er, ei = entry(even, r)
        o_r, oi = entry(odd, r)
        if r == 0:
            out.append((er + o_r, None))
            continue
        if 4 * r == n:
            re = er if oi is None else er + oi
            im = -o_r if ei is None else ei - o_r
            out.append((re, im))
            continue
        c, s = math.cos(2 * math.pi * r / n), math.sin(2 * math.pi * r / n)
        if oi is None:
            tr, ti = c * o_r, -s * o_r
        else:
            tr, ti = c * o_r + s * oi, c * oi - s * o_r
        out.append((er + tr, ti if ei is None else ei + ti))
    return out


def real_idft(hs, n):
    if n == 1:
        return [hs[0][0]]
    if n == 2:
        return [hs[0][0] + hs[1][0], hs[0][0] - hs[1][0]]
    half = n // 2
    evens, odds = [], []
    for r in range(half // 2 + 1):
        re, im = hs[r]
        mr, mi = hs[half - r]
        sum_re, dif_re = re + mr, re - mr
        if r == 0:
            evens.append((sum_re, None))
            odds.append((dif_re, None))
            continue
        if 2 * r == half:
            evens.append((sum_re, None))
            odds.append((-2.0 * im, None))
            continue
        sum_im, dif_im = im - mi, im + mi
        c, s = math.cos(2 * math.pi * r / n), math.sin(2 * math.pi * r / n)
        evens.append((sum_re, sum_im))
        odds.append((c * dif_re - s * dif_im, c * dif_im + s * dif_re))
    a, b = real_idft(evens, half), real_idft(odds, half)
    out = []
    for x, y in zip(a, b):
        out += [x, y]
    return out


def halves(x):
    hi = x.astype(BF16)
    return hi, (x - hi.astype(F32)).astype(BF16)


def fill_tables(base_ref, table):
    ca, sa = base_ref[0:16, :], base_ref[16:32, :]
    for r in range(17):
        parts = []
        for k, sign in ((r, 1.0), (32 - r, -1.0)):
            cb = base_ref[32 + k : 33 + k, :]
            sb = base_ref[72 + k : 73 + k, :]
            c = ca * cb - sa * sb
            s = sa * cb + ca * sb
            parts.append((c, s, sign))
        for p, (c, s, sign) in enumerate(parts):
            for row, half, value in (
                (32 * p, 0, c),
                (32 * p, 1, sign * s),
                (32 * p + 16, 0, -s),
                (32 * p + 16, 1, sign * c),
            ):
                hi, lo = halves(value)
                table[0, r, row : row + 16, 256 * half : 256 * half + 256] = hi
                table[1, r, row : row + 16, 256 * half : 256 * half + 256] = lo


def scale_at(r, limits):
    limit = jnp.where(lax.broadcasted_iota(jnp.int32, (8, 64), 0) < 3, limits[0], limits[1])
    n = lax.broadcasted_iota(jnp.int32, (8, 64), 1)
    mirror = n >= 32
    k = 32 * (n & 15) + jnp.where(mirror, 32 - r, r)
    keep = k <= limit
    if r in (0, 16):
        keep = keep & (n < 32)
        weight = jnp.where(k > 0, 2.0 / NLON, 1.0 / NLON)
    else:
        weight = 1.0 / NLON
    return jnp.where(keep, weight, 0.0).astype(F32)


def zonal(get, put, table, limits):
    spec = real_dft([get(c) for c in range(32)])
    nt = (((1,), (1,)), ((), ()))
    nn = (((1,), (0,)), ((), ()))

    def product(v, r, dims):
        hi, lo = halves(v)
        both = jnp.concatenate([hi, lo], axis=0)
        p = lax.dot_general(both, table[0, r], dims, preferred_element_type=F32)
        q = lax.dot_general(hi, table[1, r], dims, preferred_element_type=F32)
        return p[0:8] + p[8:16] + q

    back = []
    for r in range(17):
        re, im = spec[r]
        im = jnp.zeros_like(re) if im is None else im
        s = product(jnp.concatenate([re, im], axis=1), r, nt) * scale_at(r, limits)
        w = product(s, r, nn)
        back.append((w[:, 0:256], None if r in (0, 16) else w[:, 256:512]))
    for c, value in enumerate(real_idft(back, 32)):
        put(c, value)


def fill_base(base):
    for start, count, step in ((0, 16, 32), (32, 40, 1)):
        i = lax.broadcasted_iota(jnp.int32, (count, 256), 1)
        k = lax.broadcasted_iota(jnp.int32, (count, 256), 0) * step
        product = (i * k).astype(F32)
        turns = jnp.floor(product * (1.0 / NLON))
        phase = product - turns * NLON
        phase = jnp.where(phase < 0, phase + NLON, phase)
        phase = jnp.where(phase >= NLON, phase - NLON, phase)
        angle = phase * (TWO_PI / NLON)
        base[start : start + count, :] = jnp.where(i < 225, jnp.cos(angle), 0.0)
        base[start + count : start + 2 * count, :] = jnp.where(i < 225, jnp.sin(angle), 0.0)


def slot_table(meta_ref, band, cols, slot_ref, id_ref):
    nt = (((1,), (1,)), ((), ()))
    nb = 2 * meta_ref.shape[1]
    owner = jnp.concatenate([meta_ref[0:1, :], meta_ref[1:2, :]], axis=1) - (band - 1) * cols
    sub = lax.broadcasted_iota(jnp.int32, (nb, nb), 0)
    lane = lax.broadcasted_iota(jnp.int32, (nb, nb), 1)
    across = jnp.broadcast_to(owner, (nb, nb))
    down = jnp.transpose(across)
    earlier = jnp.where((down == across) & (sub < lane), 1, 0)
    rank = jnp.sum(earlier, axis=0, keepdims=True)
    rank_down = jnp.transpose(jnp.broadcast_to(rank, (128, nb)))
    near = down[:, 0:128] == lane[:, 0:128]
    for s in range(CAP):
        here = jnp.where(near & (rank_down == s), sub[:, 0:128], 0)
        slot_ref[s : s + 1, :] = jnp.sum(here, axis=0, keepdims=True)
    number = lax.broadcasted_iota(jnp.int32, (128, nb), 0)
    to = (jnp.broadcast_to(owner, (128, nb)) == number).astype(F32).astype(BF16)
    tile = (jnp.concatenate([meta_ref[2:3, :], meta_ref[3:4, :]], axis=1) + 1).astype(F32)
    tiles = jnp.where(jnp.broadcast_to(rank, (128, nb)) == number, tile, 0.0).astype(BF16)
    id_ref[...] = lax.dot_general(to, tiles, nt, preferred_element_type=F32) - 1.0


def kernel(
    meta_ref, src_ref, w_ref, out_ref,
    pick_ref, slot_ref, sb_ref, id_ref, wbuf, part, send, recv, data, own, dtx, drx, tiles, flat, rtx, rrx, ztx, zrx, base, table,
    in_sem, w_sem, send_sem, recv_sem, dense_sem, row_sem, pair_sem,
):
    bands = lax.axis_size("band")
    band, col = lax.axis_index("band"), lax.axis_index("col")
    z, x = col // NX, lax.rem(col, NX)
    cols = NZ * NX
    planes = {0: (0, 1), 1: (1, 5), 2: (5, 8)}

    pick_copy = pltpu.make_async_copy(meta_ref, pick_ref, in_sem.at[0])
    pick_copy.start()

    def weight_copy(g):
        return pltpu.make_async_copy(
            w_ref.at[pl.ds(g * GROUP, GROUP)], wbuf.at[pl.ds(g * GROUP, GROUP)], w_sem.at[g]
        )

    groups = wbuf.shape[0] // GROUP
    for g in range(groups):
        weight_copy(g).start()

    def valid(off):
        other = band + off - 1
        return (other >= 0) & (other < bands)

    barrier = pltpu.get_barrier_semaphore()

    def greet(c, carry):
        for off in (0, 1, 2):
            ok = c != col if off == 1 else valid(off)

            @pl.when(ok)
            def _(off=off):
                pl.semaphore_signal(barrier, inc=1, device_id=(band + off - 1, c), device_id_type=MESH)

        return carry

    lax.fori_loop(0, cols, greet, 0)

    for side, edge in ((0, 0), (2, bands - 1)):

        @pl.when(band == edge)
        def _(side=side):
            for d in range(NZ):
                first = d * 3 * NX + side * NX
                recv[first : first + NX] = jnp.full((NX, *recv.shape[1:]), -1.0, F32)

    pick_copy.wait()
    table_copy = pltpu.make_async_copy(slot_ref, sb_ref, in_sem.at[1])

    for g in range(groups):
        weight_copy(g).wait()

        def some(i, carry, g=g):
            first = g * GROUP + i * 8
            lane = g * GROUP % 128 + i * 8
            for n in range(8):
                k = first + n
                part[k] = jnp.dot(src_ref[pick_ref[4 + g * GROUP // 128, lane + n]], wbuf[k], preferred_element_type=F32)
            return carry

        lax.fori_loop(0, GROUP // 8, some, 0)
        if g == 0:
            slot_table(meta_ref, band, cols, slot_ref, id_ref)
            table_copy.start()

    def turn(parity):
        return 1 - 2 * (parity & 1)

    def route(i, off):
        u = i // NX
        delta = jnp.where(u < 4, 4 - u, lax.rem(u + 1, NZ))
        s = turn(band + off - 1)
        owner_z = lax.rem(z - s * delta + 2 * NZ, NZ)
        shift = jnp.where(delta == 0, 0, jnp.where(delta <= 4, s, -s))
        plane = lax.rem(owner_z + shift + NZ, NZ)
        to_x = lax.rem(x + i, NX)
        return owner_z * NX + to_x, delta, plane * NX + to_x

    def pack(i):
        for off in range(3):
            c, _, _ = route(i, off)
            j = off * cols + c
            for s in range(CAP):
                send[off, c, pl.ds(s, 6, stride=CAP), :] = part[sb_ref[s, j]]
            send[off, c, 36:37, :] = id_ref[pl.ds(j, 1), :]

    def transmit(i):
        for off in (0, 2, 1):
            c, delta, to = route(i, off)
            ok = to != col if off == 1 else valid(off)
            group = jnp.where(delta == 0, 0, jnp.where(delta <= 4, 1, 2))

            @pl.when(ok)
            def _(off=off, c=c, delta=delta, to=to, group=group):
                pltpu.make_async_remote_copy(
                    src_ref=send.at[off, c, 0:SENT],
                    dst_ref=recv.at[delta * 3 * NX + (2 - off) * NX + x, 0:SENT],
                    send_sem=send_sem.at[off],
                    recv_sem=recv_sem.at[group, 2 - off],
                    device_id=(band + off - 1, to),
                    device_id_type=MESH,
                ).start()

    table_copy.wait()
    pack(0)
    inner = (band > 0).astype(jnp.int32) + (band < bands - 1).astype(jnp.int32)
    pl.semaphore_wait(barrier, cols - 1 + cols * inner)

    def both(i, carry):
        @pl.when(i < cols - 1)
        def _():
            pack(i + 1)

        transmit(i)
        return carry

    lax.fori_loop(0, cols, both, 0)
    mine = turn(band)
    up = lax.rem(z + mine + NZ, NZ) * NX + x
    down = lax.rem(z - mine + NZ, NZ) * NX + x
    for c, delta, group in ((col, 0, 0), (down, 1, 1), (up, 7, 2)):
        pltpu.make_async_copy(
            send.at[1, c, 0:SENT],
            recv.at[delta * 3 * NX + NX + x, 0:SENT],
            recv_sem.at[group, 1],
        ).start()
    data[...] = jnp.zeros_like(data)
    fill_base(base)
    fill_tables(base, table)

    def take(group):
        first, last = planes[group]
        n = (last - first) * NX
        for off in range(3):
            wait = pltpu.make_async_copy(recv.at[0:n, 0:SENT], recv.at[0:n, 0:SENT], recv_sem.at[group, off])
            if off == 1:
                wait.wait()
            else:

                @pl.when(valid(off))
                def _(wait=wait):
                    wait.wait()

    def summed(group, put):
        first, last = (3 * NX * p for p in planes[group])
        n = last - first

        def lay(i, carry):
            j = first + i
            for lev in range(6):
                data[pl.ds(pl.multiple_of(j * 8, 8), 6), 128 * lev : 128 * lev + 128] = recv[
                    j, lev * CAP : lev * CAP + CAP, :
                ]
            return carry

        lax.fori_loop(0, n, lay, 0)
        ids = recv[first:last, 36:37, :].reshape(n, 1, 128)
        lane = lax.broadcasted_iota(jnp.int32, (n, 8, 128), 2)
        sub = lax.broadcasted_iota(jnp.int32, (n, 8, 128), 1)
        diag = jnp.where(lane == sub, jnp.broadcast_to(ids, (n, 8, 128)), 0.0)
        diag = diag.reshape(8 * n, 128).astype(BF16)
        spread = jnp.dot(diag, jnp.ones((128, 128), BF16), preferred_element_type=F32)
        tile = lax.broadcasted_iota(jnp.int32, (8 * n, 128), 1).astype(F32)
        chooser = (spread == tile).astype(F32).astype(BF16)
        tn = (((0,), (0,)), ((), ()))
        for h in range(2):
            hi, lo = halves(data[8 * first : 8 * last, 384 * h : 384 * h + 384])
            put(
                h,
                lax.dot_general(chooser, hi, tn, preferred_element_type=F32)
                + lax.dot_general(chooser, lo, tn, preferred_element_type=F32),
            )

    def dense(which, h, to):
        return pltpu.make_async_remote_copy(
            src_ref=dtx.at[which, 3 * h : 3 * h + 3, 0:113],
            dst_ref=drx.at[which, 3 * h : 3 * h + 3, 0:113],
            send_sem=dense_sem.at[which, h, 0],
            recv_sem=dense_sem.at[which, h, 1],
            device_id=(band, to),
            device_id_type=MESH,
        )

    def keep_own(h, total):
        own[:, 384 * h : 384 * h + 384] = total

    for group, which, to in ((1, 0, down), (0, None, None), (2, 1, up)):
        take(group)

        def pass_on(h, total, which=which, to=to):
            for lev in range(3):
                dtx[which, 3 * h + lev] = total[0:120, 128 * lev : 128 * lev + 128]
            dense(which, h, to).start()

        summed(group, keep_own if which is None else pass_on)

    def row(lat):
        t, s = divmod(225 * lat, 128)
        a, b, c = (tiles[8 * (t + n) : 8 * (t + n) + 8, :] for n in range(3))
        if s:
            a, b, c = (pltpu.roll(v, 128 - s, 1) for v in (a, b, c))
            keep = lax.broadcasted_iota(jnp.int32, (8, 128), 1) < 128 - s
            a, b = jnp.where(keep, a, b), jnp.where(keep, b, c)
        return a, b

    def swap(src, dst, which, j):
        def step(i, carry):
            u = i // NX
            m = (u + 1) // 2
            dz = jnp.where(lax.rem(u, 2) == 0, 4 + m, 4 - m)
            to = lax.rem(z + dz, NZ) * NX + lax.rem(x + i, NX)

            @pl.when(to != col)
            def _():
                pltpu.make_async_remote_copy(
                    src_ref=src.at[j, to, 0:12],
                    dst_ref=dst.at[j, col, 0:12],
                    send_sem=row_sem.at[which, j, 0],
                    recv_sem=row_sem.at[which, j, 1],
                    device_id=(band, to),
                    device_id_type=MESH,
                ).start()

            return carry

        lax.fori_loop(0, cols, step, 0)
        pltpu.make_async_copy(src.at[j, col, 0:12], dst.at[j, col, 0:12], row_sem.at[which, j, 1]).start()

    def swapped(dst, which, j):
        pltpu.make_async_copy(dst.at[j, :, 0:12], dst.at[j, :, 0:12], row_sem.at[which, j, 1]).wait()

    def swap_sent(src, which, j):
        part_of = src.at[j, 0 : cols - 1, 0:12]
        pltpu.make_async_copy(part_of, part_of, row_sem.at[which, j, 0]).wait()

    for h in range(2):
        dense(1, h, up).wait()
        dense(0, h, down).wait()
        for lev in range(3 * h, 3 * h + 3):
            tiles[pl.ds(lev, 120, stride=8), :] = (
                own[0:120, 128 * lev : 128 * lev + 128] + drx[0, lev] + drx[1, lev]
            )
        if h == 0:
            pl.semaphore_signal(
                pair_sem, inc=1, device_id=(band + turn(band), col), device_id_type=MESH
            )
        for lat in range(2 * cols):
            a, b = (v[3 * h : 3 * h + 3] for v in row(lat))
            flat[pl.ds(192 * h + lat, 3, stride=64), :] = a
            flat[pl.ds(384 + 192 * h + lat, 3, stride=64), :] = b
            first = 3 * (lat % 2)
            rtx[h, lat // 2, first : first + 3, :] = a
            rtx[h, lat // 2, 6 + first : 9 + first, :] = b
        if h == 0:
            pl.semaphore_wait(pair_sem, 1)
        swap(rtx, rrx, 0, h)
    out_ref[0, :, 0:128] = flat[0:384, :]
    out_ref[0, :, 128:225] = flat[384:768, 0:97]

    for j in range(2):
        swapped(rrx, 0, j)

        def get(c, j=j):
            return jnp.concatenate([rrx[j, c, 0:8, :], rrx[j, c, 6:14, :]], axis=1)

        def put(c, value, j=j):
            ztx[j, c, 0:6, :] = value[0:6, 0:128]
            ztx[j, c, 6:12, :] = value[0:6, 128:256]

        zonal(get, put, table, (pick_ref[6, 0], pick_ref[6, 1]))
        swap(ztx, zrx, 1, j)

    pltpu.make_async_copy(
        send.at[1, 0 : cols - 3, 0:SENT], send.at[1, 0 : cols - 3, 0:SENT], send_sem.at[1]
    ).wait()
    for off in (0, 2):

        @pl.when(valid(off))
        def _(off=off):
            pltpu.make_async_copy(send.at[off, :, 0:SENT], send.at[off, :, 0:SENT], send_sem.at[off]).wait()

    for j in range(2):
        swap_sent(rtx, 0, j)
    for j in range(2):
        swapped(zrx, 1, j)
        for lat in range(2 * cols):
            first = 3 * (lat % 2)
            flat[pl.ds(192 * j + lat, 3, stride=64), :] = zrx[j, lat // 2, first : first + 3, :]
            flat[pl.ds(384 + 192 * j + lat, 3, stride=64), :] = zrx[j, lat // 2, 6 + first : 9 + first, :]
    out_ref[1, :, 0:128] = flat[0:384, :]
    out_ref[1, :, 128:225] = flat[384:768, 0:97]
    for j in range(2):
        swap_sent(ztx, 1, j)


def local(source, weights, source_block, owner_device, target_tile, cutoff):
    cols = lax.axis_size("col")
    levels, nb, width = 6, weights.shape[0], weights.shape[1]
    blocks = jnp.transpose(source.reshape(levels, -1, width), (1, 0, 2))
    spare = jnp.zeros((nb - cutoff.shape[0],), jnp.int32)
    meta = jnp.concatenate([owner_device[:, 0], target_tile, source_block, cutoff, spare]).reshape(8, nb // 2)
    vmem = pl.BlockSpec(memory_space=pltpu.VMEM)
    rows = (2, cols, 16, 128)
    both = pl.pallas_call(
        kernel,
        name="remap",
        out_shape=jax.ShapeDtypeStruct((2, 384, 225), F32),
        in_specs=[vmem, vmem, pl.BlockSpec(memory_space=pl.ANY)],
        out_specs=vmem,
        scratch_shapes=[
            pltpu.SMEM((8, nb // 2), jnp.int32),
            pltpu.VMEM((8, 128), jnp.int32),
            pltpu.SMEM((8, 128), jnp.int32),
            pltpu.VMEM((128, 128), F32),
            pltpu.VMEM((nb, width, width), BF16),
            pltpu.VMEM((nb, 6, 128), F32),
            pltpu.VMEM((3, cols, ROWS, 128), F32),
            pltpu.VMEM((3 * cols, ROWS, 128), F32),
            pltpu.VMEM((24 * cols, 768), F32),
            pltpu.VMEM((128, 768), F32),
            pltpu.VMEM((2, 6, 120, 128), F32),
            pltpu.VMEM((2, 6, 120, 128), F32),
            pltpu.VMEM((1024, 128), F32),
            pltpu.VMEM((768, 128), F32),
            pltpu.VMEM(rows, F32),
            pltpu.VMEM(rows, F32),
            pltpu.VMEM(rows, F32),
            pltpu.VMEM(rows, F32),
            pltpu.VMEM((112, 256), F32),
            pltpu.VMEM((2, 17, 64, 512), BF16),
            pltpu.SemaphoreType.DMA((2,)),
            pltpu.SemaphoreType.DMA((nb // GROUP,)),
            pltpu.SemaphoreType.DMA((3,)),
            pltpu.SemaphoreType.DMA((3, 3)),
            pltpu.SemaphoreType.DMA((2, 2, 2)),
            pltpu.SemaphoreType.DMA((2, 2, 2)),
            pltpu.SemaphoreType.REGULAR,
        ],
        compiler_params=pltpu.CompilerParams(
            collective_id=0, has_side_effects=True, vmem_limit_bytes=50 * 2**20
        ),
    )(meta, blocks, weights)
    return both[0].reshape(6, 64, 225), both[1].reshape(6, 64, 225)


def solution(mesh):
    in_specs = (
        P(None, ("band", "col")),
        P(("band", "col"), None, None),
        P(("band", "col")),
        P(("band", "col"), None),
        P(("band", "col")),
        P(("band", "col")),
    )
    out_specs = (P(None, "band", "col"), P(None, "band", "col"))
    return jax.shard_map(local, mesh=mesh, in_specs=in_specs, out_specs=out_specs, check_vma=False)
```

```python
import functools
import math

import jax
import jax.numpy as jnp
from jax import lax
from jax.experimental import pallas as pl
from jax.experimental.pallas import tpu as pltpu
from jax.sharding import PartitionSpec as P

NLON = 7200
KW = 512
CAP = 6
ROWS = 40
SENT = 37
TWO_PI = 6.283185307179586
MESH = pl.DeviceIdType.MESH
F32 = jnp.float32
BF16 = jnp.bfloat16
NZ, NX = 8, 4
GROUP = 32


def real_dft(xs):
    n = len(xs)
    if n == 1:
        return [(xs[0], None)]
    if n == 2:
        return [(xs[0] + xs[1], None), (xs[0] - xs[1], None)]
    even, odd = real_dft(xs[0::2]), real_dft(xs[1::2])
    half = n // 2

    def entry(spec, r):
        if r <= half // 2:
            re, im = spec[r]
            return re, im
        re, im = spec[half - r]
        return re, (None if im is None else -im)

    out = []
    for r in range(half + 1):
        if r == half:
            out.append((even[0][0] - odd[0][0], None))
            continue
        er, ei = entry(even, r)
        o_r, oi = entry(odd, r)
        if r == 0:
            out.append((er + o_r, None))
            continue
        if 4 * r == n:
            re = er if oi is None else er + oi
            im = -o_r if ei is None else ei - o_r
            out.append((re, im))
            continue
        c, s = math.cos(2 * math.pi * r / n), math.sin(2 * math.pi * r / n)
        if oi is None:
            tr, ti = c * o_r, -s * o_r
        else:
            tr, ti = c * o_r + s * oi, c * oi - s * o_r
        out.append((er + tr, ti if ei is None else ei + ti))
    return out


def real_idft(hs, n):
    if n == 1:
        return [hs[0][0]]
    if n == 2:
        return [hs[0][0] + hs[1][0], hs[0][0] - hs[1][0]]
    half = n // 2
    evens, odds = [], []
    for r in range(half // 2 + 1):
        re, im = hs[r]
        mr, mi = hs[half - r]
        sum_re, dif_re = re + mr, re - mr
        if r == 0:
            evens.append((sum_re, None))
            odds.append((dif_re, None))
            continue
        if 2 * r == half:
            evens.append((sum_re, None))
            odds.append((-2.0 * im, None))
            continue
        sum_im, dif_im = im - mi, im + mi
        c, s = math.cos(2 * math.pi * r / n), math.sin(2 * math.pi * r / n)
        evens.append((sum_re, sum_im))
        odds.append((c * dif_re - s * dif_im, c * dif_im + s * dif_re))
    a, b = real_idft(evens, half), real_idft(odds, half)
    out = []
    for x, y in zip(a, b):
        out += [x, y]
    return out


def halves(x):
    hi = x.astype(BF16)
    return hi, (x - hi.astype(F32)).astype(BF16)


def fill_tables(base_ref, table):
    ca, sa = base_ref[0:16, :], base_ref[16:32, :]
    for r in range(17):
        parts = []
        for k, sign in ((r, 1.0), (32 - r, -1.0)):
            cb = base_ref[32 + k : 33 + k, :]
            sb = base_ref[72 + k : 73 + k, :]
            c = ca * cb - sa * sb
            s = sa * cb + ca * sb
            parts.append((c, s, sign))
        for p, (c, s, sign) in enumerate(parts):
            for row, half, value in (
                (32 * p, 0, c),
                (32 * p, 1, sign * s),
                (32 * p + 16, 0, -s),
                (32 * p + 16, 1, sign * c),
            ):
                hi, lo = halves(value)
                table[0, r, row : row + 16, 256 * half : 256 * half + 256] = hi
                table[1, r, row : row + 16, 256 * half : 256 * half + 256] = lo


def scale_at(r, limits):
    limit = jnp.where(lax.broadcasted_iota(jnp.int32, (8, 64), 0) < 3, limits[0], limits[1])
    n = lax.broadcasted_iota(jnp.int32, (8, 64), 1)
    mirror = n >= 32
    k = 32 * (n & 15) + jnp.where(mirror, 32 - r, r)
    keep = k <= limit
    if r in (0, 16):
        keep = keep & (n < 32)
        weight = jnp.where(k > 0, 2.0 / NLON, 1.0 / NLON)
    else:
        weight = 1.0 / NLON
    return jnp.where(keep, weight, 0.0).astype(F32)


def zonal(get, put, table, limits):
    spec = real_dft([get(c) for c in range(32)])
    nt = (((1,), (1,)), ((), ()))
    nn = (((1,), (0,)), ((), ()))

    def product(v, r, dims):
        hi, lo = halves(v)
        both = jnp.concatenate([hi, lo], axis=0)
        p = lax.dot_general(both, table[0, r], dims, preferred_element_type=F32)
        q = lax.dot_general(hi, table[1, r], dims, preferred_element_type=F32)
        return p[0:8] + p[8:16] + q

    back = []
    for r in range(17):
        re, im = spec[r]
        im = jnp.zeros_like(re) if im is None else im
        s = product(jnp.concatenate([re, im], axis=1), r, nt) * scale_at(r, limits)
        w = product(s, r, nn)
        back.append((w[:, 0:256], None if r in (0, 16) else w[:, 256:512]))
    for c, value in enumerate(real_idft(back, 32)):
        put(c, value)


def fill_base(base):
    for start, count, step in ((0, 16, 32), (32, 40, 1)):
        i = lax.broadcasted_iota(jnp.int32, (count, 256), 1)
        k = lax.broadcasted_iota(jnp.int32, (count, 256), 0) * step
        product = (i * k).astype(F32)
        turns = jnp.floor(product * (1.0 / NLON))
        phase = product - turns * NLON
        phase = jnp.where(phase < 0, phase + NLON, phase)
        phase = jnp.where(phase >= NLON, phase - NLON, phase)
        angle = phase * (TWO_PI / NLON)
        base[start : start + count, :] = jnp.where(i < 225, jnp.cos(angle), 0.0)
        base[start + count : start + 2 * count, :] = jnp.where(i < 225, jnp.sin(angle), 0.0)


def slot_table(meta_ref, band, cols, slot_ref, id_ref):
    nt = (((1,), (1,)), ((), ()))
    nb = 2 * meta_ref.shape[1]
    owner = jnp.concatenate([meta_ref[0:1, :], meta_ref[1:2, :]], axis=1) - (band - 1) * cols
    sub = lax.broadcasted_iota(jnp.int32, (nb, nb), 0)
    lane = lax.broadcasted_iota(jnp.int32, (nb, nb), 1)
    across = jnp.broadcast_to(owner, (nb, nb))
    down = jnp.transpose(across)
    earlier = jnp.where((down == across) & (sub < lane), 1, 0)
    rank = jnp.sum(earlier, axis=0, keepdims=True)
    rank_down = jnp.transpose(jnp.broadcast_to(rank, (128, nb)))
    near = down[:, 0:128] == lane[:, 0:128]
    for s in range(CAP):
        here = jnp.where(near & (rank_down == s), sub[:, 0:128], 0)
        slot_ref[s : s + 1, :] = jnp.sum(here, axis=0, keepdims=True)
    number = lax.broadcasted_iota(jnp.int32, (128, nb), 0)
    to = (jnp.broadcast_to(owner, (128, nb)) == number).astype(F32).astype(BF16)
    tile = (jnp.concatenate([meta_ref[2:3, :], meta_ref[3:4, :]], axis=1) + 1).astype(F32)
    tiles = jnp.where(jnp.broadcast_to(rank, (128, nb)) == number, tile, 0.0).astype(BF16)
    id_ref[...] = lax.dot_general(to, tiles, nt, preferred_element_type=F32) - 1.0


def kernel(
    meta_ref, src_ref, w_ref, out_ref,
    pick_ref, slot_ref, sb_ref, id_ref, wbuf, part, send, recv, data, own, dtx, drx, tiles, flat, rtx, rrx, ztx, zrx, base, table,
    in_sem, w_sem, send_sem, recv_sem, dense_sem, row_sem, pair_sem,
):
    bands = lax.axis_size("band")
    band, col = lax.axis_index("band"), lax.axis_index("col")
    z, x = col // NX, lax.rem(col, NX)
    cols = NZ * NX
    planes = {0: (0, 1), 1: (2, 5), 2: (5, 8), 3: (1, 2)}

    pick_copy = pltpu.make_async_copy(meta_ref, pick_ref, in_sem.at[0])
    pick_copy.start()

    def weight_copy(g):
        return pltpu.make_async_copy(
            w_ref.at[pl.ds(g * GROUP, GROUP)], wbuf.at[pl.ds(g * GROUP, GROUP)], w_sem.at[g]
        )

    groups = wbuf.shape[0] // GROUP
    for g in range(groups):
        weight_copy(g).start()

    def valid(off):
        other = band + off - 1
        return (other >= 0) & (other < bands)

    barrier = pltpu.get_barrier_semaphore()

    def greet(c, carry):
        for off in (0, 1, 2):
            ok = c != col if off == 1 else valid(off)

            @pl.when(ok)
            def _(off=off):
                pl.semaphore_signal(barrier, inc=1, device_id=(band + off - 1, c), device_id_type=MESH)

        return carry

    lax.fori_loop(0, cols, greet, 0)

    for side, edge in ((0, 0), (2, bands - 1)):

        @pl.when(band == edge)
        def _(side=side):
            for d in range(NZ):
                first = d * 3 * NX + side * NX
                recv[first : first + NX] = jnp.full((NX, *recv.shape[1:]), -1.0, F32)

    pick_copy.wait()
    table_copy = pltpu.make_async_copy(slot_ref, sb_ref, in_sem.at[1])

    for g in range(groups):
        weight_copy(g).wait()

        def some(i, carry, g=g):
            first = g * GROUP + i * 8
            lane = g * GROUP % 128 + i * 8
            for n in range(8):
                k = first + n
                part[k] = jnp.dot(src_ref[pick_ref[4 + g * GROUP // 128, lane + n]], wbuf[k], preferred_element_type=F32)
            return carry

        lax.fori_loop(0, GROUP // 8, some, 0)
        if g == 0:
            slot_table(meta_ref, band, cols, slot_ref, id_ref)
            table_copy.start()

    def turn(parity):
        return 1 - 2 * (parity & 1)

    def route(i, off):
        u = i // NX
        delta = jnp.where(u < 3, 4 - u, jnp.where(u == 3, 5, jnp.where(u == 4, 1, lax.rem(u + 1, NZ))))
        s = turn(band + off - 1)
        owner_z = lax.rem(z - s * delta + 2 * NZ, NZ)
        shift = jnp.where(delta <= 1, delta * s, jnp.where(delta <= 4, 2 * s, -s))
        plane = lax.rem(owner_z + shift + NZ, NZ)
        to_x = lax.rem(x + i, NX)
        return owner_z * NX + to_x, delta, plane * NX + to_x

    def pack(i):
        for off in range(3):
            c, _, _ = route(i, off)
            j = off * cols + c
            for s in range(CAP):
                send[off, c, pl.ds(s, 6, stride=CAP), :] = part[sb_ref[s, j]]
            send[off, c, 36:37, :] = id_ref[pl.ds(j, 1), :]

    def transmit(i):
        for off in (0, 2, 1):
            c, delta, to = route(i, off)
            ok = to != col if off == 1 else valid(off)
            group = jnp.where(delta <= 1, 3 * delta, jnp.where(delta <= 4, 1, 2))

            @pl.when(ok)
            def _(off=off, c=c, delta=delta, to=to, group=group):
                pltpu.make_async_remote_copy(
                    src_ref=send.at[off, c, 0:SENT],
                    dst_ref=recv.at[delta * 3 * NX + (2 - off) * NX + x, 0:SENT],
                    send_sem=send_sem.at[off],
                    recv_sem=recv_sem.at[group, 2 - off],
                    device_id=(band + off - 1, to),
                    device_id_type=MESH,
                ).start()

    table_copy.wait()
    pack(0)
    inner = (band > 0).astype(jnp.int32) + (band < bands - 1).astype(jnp.int32)
    pl.semaphore_wait(barrier, cols - 1 + cols * inner)

    def both(i, carry):
        @pl.when(i < cols - 1)
        def _():
            pack(i + 1)

        transmit(i)
        return carry

    lax.fori_loop(0, cols, both, 0)
    mine = turn(band)
    up = lax.rem(z + mine + NZ, NZ) * NX + x
    down = lax.rem(z - mine + NZ, NZ) * NX + x
    down2 = lax.rem(z - 2 * mine + NZ, NZ) * NX + x
    for c, delta, group in ((col, 0, 0), (down, 1, 3), (down2, 2, 1), (up, 7, 2)):
        pltpu.make_async_copy(
            send.at[1, c, 0:SENT],
            recv.at[delta * 3 * NX + NX + x, 0:SENT],
            recv_sem.at[group, 1],
        ).start()
    data[...] = jnp.zeros_like(data)
    fill_base(base)
    fill_tables(base, table)

    def take(group):
        first, last = planes[group]
        n = (last - first) * NX
        for off in range(3):
            wait = pltpu.make_async_copy(recv.at[0:n, 0:SENT], recv.at[0:n, 0:SENT], recv_sem.at[group, off])
            if off == 1:
                wait.wait()
            else:

                @pl.when(valid(off))
                def _(wait=wait):
                    wait.wait()

    def summed(group, put):
        first, last = (3 * NX * p for p in planes[group])
        n = last - first

        def lay(i, carry):
            j = first + i
            for lev in range(6):
                data[pl.ds(pl.multiple_of(j * 8, 8), 6), 128 * lev : 128 * lev + 128] = recv[
                    j, lev * CAP : lev * CAP + CAP, :
                ]
            return carry

        lax.fori_loop(0, n, lay, 0)
        ids = recv[first:last, 36:37, :].reshape(n, 1, 128)
        lane = lax.broadcasted_iota(jnp.int32, (n, 8, 128), 2)
        sub = lax.broadcasted_iota(jnp.int32, (n, 8, 128), 1)
        diag = jnp.where(lane == sub, jnp.broadcast_to(ids, (n, 8, 128)), 0.0)
        diag = diag.reshape(8 * n, 128).astype(BF16)
        spread = jnp.dot(diag, jnp.ones((128, 128), BF16), preferred_element_type=F32)
        tile = lax.broadcasted_iota(jnp.int32, (8 * n, 128), 1).astype(F32)
        chooser = (spread == tile).astype(F32).astype(BF16)
        tn = (((0,), (0,)), ((), ()))
        for h in range(2):
            hi, lo = halves(data[8 * first : 8 * last, 384 * h : 384 * h + 384])
            put(
                h,
                lax.dot_general(chooser, hi, tn, preferred_element_type=F32)
                + lax.dot_general(chooser, lo, tn, preferred_element_type=F32),
            )

    def dense(which, h, to):
        return pltpu.make_async_remote_copy(
            src_ref=dtx.at[which, 3 * h : 3 * h + 3, 0:113],
            dst_ref=drx.at[which, 3 * h : 3 * h + 3, 0:113],
            send_sem=dense_sem.at[which, h, 0],
            recv_sem=dense_sem.at[which, h, 1],
            device_id=(band, to),
            device_id_type=MESH,
        )

    def keep(h, total):
        own[:, 384 * h : 384 * h + 384] = total

    def pass_on(which, to):
        def put(h, total):
            for lev in range(3):
                dtx[which, 3 * h + lev] = total[0:120, 128 * lev : 128 * lev + 128]
            dense(which, h, to).start()

        return put

    take(1)
    summed(1, pass_on(2, down))
    take(3)
    summed(3, keep)
    for h in range(2):
        dense(2, h, down).wait()
        for lev in range(3 * h, 3 * h + 3):
            dtx[0, lev] = own[0:120, 128 * lev : 128 * lev + 128] + drx[2, lev]
        dense(0, h, down).start()
    take(2)
    summed(2, pass_on(1, up))
    take(0)
    summed(0, keep)

    def row(lat):
        t, s = divmod(225 * lat, 128)
        a, b, c = (tiles[8 * (t + n) : 8 * (t + n) + 8, :] for n in range(3))
        if s:
            a, b, c = (pltpu.roll(v, 128 - s, 1) for v in (a, b, c))
            keep = lax.broadcasted_iota(jnp.int32, (8, 128), 1) < 128 - s
            a, b = jnp.where(keep, a, b), jnp.where(keep, b, c)
        return a, b

    def swap(src, dst, which, j):
        def step(i, carry):
            u = i // NX
            m = (u + 1) // 2
            dz = jnp.where(lax.rem(u, 2) == 0, 4 + m, 4 - m)
            to = lax.rem(z + dz, NZ) * NX + lax.rem(x + i, NX)

            @pl.when(to != col)
            def _():
                pltpu.make_async_remote_copy(
                    src_ref=src.at[j, to, 0:12],
                    dst_ref=dst.at[j, col, 0:12],
                    send_sem=row_sem.at[which, j, 0],
                    recv_sem=row_sem.at[which, j, 1],
                    device_id=(band, to),
                    device_id_type=MESH,
                ).start()

            return carry

        lax.fori_loop(0, cols, step, 0)
        pltpu.make_async_copy(src.at[j, col, 0:12], dst.at[j, col, 0:12], row_sem.at[which, j, 1]).start()

    def swapped(dst, which, j):
        pltpu.make_async_copy(dst.at[j, :, 0:12], dst.at[j, :, 0:12], row_sem.at[which, j, 1]).wait()

    def swap_sent(src, which, j):
        part_of = src.at[j, 0 : cols - 1, 0:12]
        pltpu.make_async_copy(part_of, part_of, row_sem.at[which, j, 0]).wait()

    for h in range(2):
        dense(1, h, up).wait()
        dense(0, h, down).wait()
        for lev in range(3 * h, 3 * h + 3):
            tiles[pl.ds(lev, 120, stride=8), :] = (
                own[0:120, 128 * lev : 128 * lev + 128] + drx[0, lev] + drx[1, lev]
            )
        if h == 0:
            pl.semaphore_signal(
                pair_sem, inc=1, device_id=(band + turn(band), col), device_id_type=MESH
            )
        for lat in range(2 * cols):
            a, b = (v[3 * h : 3 * h + 3] for v in row(lat))
            flat[pl.ds(192 * h + lat, 3, stride=64), :] = a
            flat[pl.ds(384 + 192 * h + lat, 3, stride=64), :] = b
            first = 3 * (lat % 2)
            rtx[h, lat // 2, first : first + 3, :] = a
            rtx[h, lat // 2, 6 + first : 9 + first, :] = b
        if h == 0:
            pl.semaphore_wait(pair_sem, 1)
        swap(rtx, rrx, 0, h)
    out_ref[0, :, 0:128] = flat[0:384, :]
    out_ref[0, :, 128:225] = flat[384:768, 0:97]

    for j in range(2):
        swapped(rrx, 0, j)

        def get(c, j=j):
            return jnp.concatenate([rrx[j, c, 0:8, :], rrx[j, c, 6:14, :]], axis=1)

        def put(c, value, j=j):
            ztx[j, c, 0:6, :] = value[0:6, 0:128]
            ztx[j, c, 6:12, :] = value[0:6, 128:256]

        zonal(get, put, table, (pick_ref[6, 0], pick_ref[6, 1]))
        swap(ztx, zrx, 1, j)

    pltpu.make_async_copy(
        send.at[1, 0 : cols - 4, 0:SENT], send.at[1, 0 : cols - 4, 0:SENT], send_sem.at[1]
    ).wait()
    for off in (0, 2):

        @pl.when(valid(off))
        def _(off=off):
            pltpu.make_async_copy(send.at[off, :, 0:SENT], send.at[off, :, 0:SENT], send_sem.at[off]).wait()

    for j in range(2):
        swap_sent(rtx, 0, j)
    for j in range(2):
        swapped(zrx, 1, j)
        for lat in range(2 * cols):
            first = 3 * (lat % 2)
            flat[pl.ds(192 * j + lat, 3, stride=64), :] = zrx[j, lat // 2, first : first + 3, :]
            flat[pl.ds(384 + 192 * j + lat, 3, stride=64), :] = zrx[j, lat // 2, 6 + first : 9 + first, :]
    out_ref[1, :, 0:128] = flat[0:384, :]
    out_ref[1, :, 128:225] = flat[384:768, 0:97]
    for j in range(2):
        swap_sent(ztx, 1, j)


def local(source, weights, source_block, owner_device, target_tile, cutoff):
    cols = lax.axis_size("col")
    levels, nb, width = 6, weights.shape[0], weights.shape[1]
    blocks = jnp.transpose(source.reshape(levels, -1, width), (1, 0, 2))
    spare = jnp.zeros((nb - cutoff.shape[0],), jnp.int32)
    meta = jnp.concatenate([owner_device[:, 0], target_tile, source_block, cutoff, spare]).reshape(8, nb // 2)
    vmem = pl.BlockSpec(memory_space=pltpu.VMEM)
    rows = (2, cols, 16, 128)
    both = pl.pallas_call(
        kernel,
        name="remap",
        out_shape=jax.ShapeDtypeStruct((2, 384, 225), F32),
        in_specs=[vmem, vmem, pl.BlockSpec(memory_space=pl.ANY)],
        out_specs=vmem,
        scratch_shapes=[
            pltpu.SMEM((8, nb // 2), jnp.int32),
            pltpu.VMEM((8, 128), jnp.int32),
            pltpu.SMEM((8, 128), jnp.int32),
            pltpu.VMEM((128, 128), F32),
            pltpu.VMEM((nb, width, width), BF16),
            pltpu.VMEM((nb, 6, 128), F32),
            pltpu.VMEM((3, cols, ROWS, 128), F32),
            pltpu.VMEM((3 * cols, ROWS, 128), F32),
            pltpu.VMEM((24 * cols, 768), F32),
            pltpu.VMEM((128, 768), F32),
            pltpu.VMEM((3, 6, 120, 128), F32),
            pltpu.VMEM((3, 6, 120, 128), F32),
            pltpu.VMEM((1024, 128), F32),
            pltpu.VMEM((768, 128), F32),
            pltpu.VMEM(rows, F32),
            pltpu.VMEM(rows, F32),
            pltpu.VMEM(rows, F32),
            pltpu.VMEM(rows, F32),
            pltpu.VMEM((112, 256), F32),
            pltpu.VMEM((2, 17, 64, 512), BF16),
            pltpu.SemaphoreType.DMA((2,)),
            pltpu.SemaphoreType.DMA((nb // GROUP,)),
            pltpu.SemaphoreType.DMA((3,)),
            pltpu.SemaphoreType.DMA((4, 3)),
            pltpu.SemaphoreType.DMA((3, 2, 2)),
            pltpu.SemaphoreType.DMA((2, 2, 2)),
            pltpu.SemaphoreType.REGULAR,
        ],
        compiler_params=pltpu.CompilerParams(
            collective_id=0, has_side_effects=True, vmem_limit_bytes=50 * 2**20
        ),
    )(meta, blocks, weights)
    return both[0].reshape(6, 64, 225), both[1].reshape(6, 64, 225)


def solution(mesh):
    in_specs = (
        P(None, ("band", "col")),
        P(("band", "col"), None, None),
        P(("band", "col")),
        P(("band", "col"), None),
        P(("band", "col")),
        P(("band", "col")),
    )
    out_specs = (P(None, "band", "col"), P(None, "band", "col"))
    return jax.shard_map(local, mesh=mesh, in_specs=in_specs, out_specs=out_specs, check_vma=False)
```

```python
import functools
import math

import jax
import jax.numpy as jnp
from jax import lax
from jax.experimental import pallas as pl
from jax.experimental.pallas import tpu as pltpu
from jax.sharding import PartitionSpec as P

NLON = 7200
KW = 512
CAP = 6
ROWS = 40
SENT = 37
TWO_PI = 6.283185307179586
MESH = pl.DeviceIdType.MESH
F32 = jnp.float32
BF16 = jnp.bfloat16
NZ, NX = 8, 4
GROUP = 32


def real_dft(xs):
    n = len(xs)
    if n == 1:
        return [(xs[0], None)]
    if n == 2:
        return [(xs[0] + xs[1], None), (xs[0] - xs[1], None)]
    even, odd = real_dft(xs[0::2]), real_dft(xs[1::2])
    half = n // 2

    def entry(spec, r):
        if r <= half // 2:
            re, im = spec[r]
            return re, im
        re, im = spec[half - r]
        return re, (None if im is None else -im)

    out = []
    for r in range(half + 1):
        if r == half:
            out.append((even[0][0] - odd[0][0], None))
            continue
        er, ei = entry(even, r)
        o_r, oi = entry(odd, r)
        if r == 0:
            out.append((er + o_r, None))
            continue
        if 4 * r == n:
            re = er if oi is None else er + oi
            im = -o_r if ei is None else ei - o_r
            out.append((re, im))
            continue
        c, s = math.cos(2 * math.pi * r / n), math.sin(2 * math.pi * r / n)
        if oi is None:
            tr, ti = c * o_r, -s * o_r
        else:
            tr, ti = c * o_r + s * oi, c * oi - s * o_r
        out.append((er + tr, ti if ei is None else ei + ti))
    return out


def real_idft(hs, n):
    if n == 1:
        return [hs[0][0]]
    if n == 2:
        return [hs[0][0] + hs[1][0], hs[0][0] - hs[1][0]]
    half = n // 2
    evens, odds = [], []
    for r in range(half // 2 + 1):
        re, im = hs[r]
        mr, mi = hs[half - r]
        sum_re, dif_re = re + mr, re - mr
        if r == 0:
            evens.append((sum_re, None))
            odds.append((dif_re, None))
            continue
        if 2 * r == half:
            evens.append((sum_re, None))
            odds.append((-2.0 * im, None))
            continue
        sum_im, dif_im = im - mi, im + mi
        c, s = math.cos(2 * math.pi * r / n), math.sin(2 * math.pi * r / n)
        evens.append((sum_re, sum_im))
        odds.append((c * dif_re - s * dif_im, c * dif_im + s * dif_re))
    a, b = real_idft(evens, half), real_idft(odds, half)
    out = []
    for x, y in zip(a, b):
        out += [x, y]
    return out


def halves(x):
    hi = x.astype(BF16)
    return hi, (x - hi.astype(F32)).astype(BF16)


def fill_tables(base_ref, table):
    ca, sa = base_ref[0:16, :], base_ref[16:32, :]
    for r in range(17):
        parts = []
        for k, sign in ((r, 1.0), (32 - r, -1.0)):
            cb = base_ref[32 + k : 33 + k, :]
            sb = base_ref[72 + k : 73 + k, :]
            c = ca * cb - sa * sb
            s = sa * cb + ca * sb
            parts.append((c, s, sign))
        for p, (c, s, sign) in enumerate(parts):
            for row, half, value in (
                (32 * p, 0, c),
                (32 * p, 1, sign * s),
                (32 * p + 16, 0, -s),
                (32 * p + 16, 1, sign * c),
            ):
                hi, lo = halves(value)
                table[0, r, row : row + 16, 256 * half : 256 * half + 256] = hi
                table[1, r, row : row + 16, 256 * half : 256 * half + 256] = lo


def scale_at(r, limits):
    limit = jnp.where(lax.broadcasted_iota(jnp.int32, (8, 64), 0) < 3, limits[0], limits[1])
    n = lax.broadcasted_iota(jnp.int32, (8, 64), 1)
    mirror = n >= 32
    k = 32 * (n & 15) + jnp.where(mirror, 32 - r, r)
    keep = k <= limit
    if r in (0, 16):
        keep = keep & (n < 32)
        weight = jnp.where(k > 0, 2.0 / NLON, 1.0 / NLON)
    else:
        weight = 1.0 / NLON
    return jnp.where(keep, weight, 0.0).astype(F32)


def zonal(get, put, table, limits):
    spec = real_dft([get(c) for c in range(32)])
    nt = (((1,), (1,)), ((), ()))
    nn = (((1,), (0,)), ((), ()))

    def product(v, r, dims):
        hi, lo = halves(v)
        both = jnp.concatenate([hi, lo], axis=0)
        p = lax.dot_general(both, table[0, r], dims, preferred_element_type=F32)
        q = lax.dot_general(hi, table[1, r], dims, preferred_element_type=F32)
        return p[0:8] + p[8:16] + q

    back = []
    for r in range(17):
        re, im = spec[r]
        im = jnp.zeros_like(re) if im is None else im
        s = product(jnp.concatenate([re, im], axis=1), r, nt) * scale_at(r, limits)
        w = product(s, r, nn)
        back.append((w[:, 0:256], None if r in (0, 16) else w[:, 256:512]))
    for c, value in enumerate(real_idft(back, 32)):
        put(c, value)


def fill_base(base):
    for start, count, step in ((0, 16, 32), (32, 40, 1)):
        i = lax.broadcasted_iota(jnp.int32, (count, 256), 1)
        k = lax.broadcasted_iota(jnp.int32, (count, 256), 0) * step
        product = (i * k).astype(F32)
        turns = jnp.floor(product * (1.0 / NLON))
        phase = product - turns * NLON
        phase = jnp.where(phase < 0, phase + NLON, phase)
        phase = jnp.where(phase >= NLON, phase - NLON, phase)
        angle = phase * (TWO_PI / NLON)
        base[start : start + count, :] = jnp.where(i < 225, jnp.cos(angle), 0.0)
        base[start + count : start + 2 * count, :] = jnp.where(i < 225, jnp.sin(angle), 0.0)


def slot_table(meta_ref, band, cols, slot_ref, id_ref):
    nt = (((1,), (1,)), ((), ()))
    nb = 2 * meta_ref.shape[1]
    owner = jnp.concatenate([meta_ref[0:1, :], meta_ref[1:2, :]], axis=1) - (band - 1) * cols
    sub = lax.broadcasted_iota(jnp.int32, (nb, nb), 0)
    lane = lax.broadcasted_iota(jnp.int32, (nb, nb), 1)
    across = jnp.broadcast_to(owner, (nb, nb))
    down = jnp.transpose(across)
    earlier = jnp.where((down == across) & (sub < lane), 1, 0)
    rank = jnp.sum(earlier, axis=0, keepdims=True)
    rank_down = jnp.transpose(jnp.broadcast_to(rank, (128, nb)))
    near = down[:, 0:128] == lane[:, 0:128]
    for s in range(CAP):
        here = jnp.where(near & (rank_down == s), sub[:, 0:128], 0)
        slot_ref[s : s + 1, :] = jnp.sum(here, axis=0, keepdims=True)
    number = lax.broadcasted_iota(jnp.int32, (128, nb), 0)
    to = (jnp.broadcast_to(owner, (128, nb)) == number).astype(F32).astype(BF16)
    tile = (jnp.concatenate([meta_ref[2:3, :], meta_ref[3:4, :]], axis=1) + 1).astype(F32)
    tiles = jnp.where(jnp.broadcast_to(rank, (128, nb)) == number, tile, 0.0).astype(BF16)
    id_ref[...] = lax.dot_general(to, tiles, nt, preferred_element_type=F32) - 1.0


def kernel(
    meta_ref, src_ref, w_ref, out_ref,
    pick_ref, slot_ref, sb_ref, id_ref, wbuf, part, send, recv, data, own, dtx, drx, tiles, flat, rtx, rrx, ztx, zrx, base, table,
    in_sem, w_sem, send_sem, recv_sem, dense_sem, row_sem, pair_sem,
):
    bands = lax.axis_size("band")
    band, col = lax.axis_index("band"), lax.axis_index("col")
    z, x = col // NX, lax.rem(col, NX)
    cols = NZ * NX
    planes = {0: (0, 1), 1: (2, 5), 2: (5, 8), 3: (1, 2)}

    pick_copy = pltpu.make_async_copy(meta_ref, pick_ref, in_sem.at[0])
    pick_copy.start()

    def weight_copy(g):
        return pltpu.make_async_copy(
            w_ref.at[pl.ds(g * GROUP, GROUP)], wbuf.at[pl.ds(g * GROUP, GROUP)], w_sem.at[g]
        )

    groups = wbuf.shape[0] // GROUP
    for g in range(groups):
        weight_copy(g).start()

    def valid(off):
        other = band + off - 1
        return (other >= 0) & (other < bands)

    barrier = pltpu.get_barrier_semaphore()

    def greet(c, carry):
        for off in (0, 1, 2):
            ok = c != col if off == 1 else valid(off)

            @pl.when(ok)
            def _(off=off):
                pl.semaphore_signal(barrier, inc=1, device_id=(band + off - 1, c), device_id_type=MESH)

        return carry

    lax.fori_loop(0, cols, greet, 0)

    for side, edge in ((0, 0), (2, bands - 1)):

        @pl.when(band == edge)
        def _(side=side):
            for d in range(NZ):
                first = d * 3 * NX + side * NX
                recv[first : first + NX] = jnp.full((NX, *recv.shape[1:]), -1.0, F32)

    pick_copy.wait()
    table_copy = pltpu.make_async_copy(slot_ref, sb_ref, in_sem.at[1])

    for g in range(groups):
        weight_copy(g).wait()

        def some(i, carry, g=g):
            first = g * GROUP + i * 8
            lane = g * GROUP % 128 + i * 8
            for n in range(8):
                k = first + n
                part[k] = jnp.dot(src_ref[pick_ref[4 + g * GROUP // 128, lane + n]], wbuf[k], preferred_element_type=F32)
            return carry

        lax.fori_loop(0, GROUP // 8, some, 0)
        if g == 0:
            slot_table(meta_ref, band, cols, slot_ref, id_ref)
            table_copy.start()

    def turn(parity):
        return 1 - 2 * (parity & 1)

    def route(i, off):
        u = i // NX
        delta = jnp.where(u < 3, 4 - u, jnp.where(u == 3, 5, jnp.where(u == 4, 1, lax.rem(u + 1, NZ))))
        s = turn(band + off - 1)
        owner_z = lax.rem(z - s * delta + 2 * NZ, NZ)
        shift = jnp.where(delta <= 1, delta * s, jnp.where(delta <= 4, 2 * s, -s))
        plane = lax.rem(owner_z + shift + NZ, NZ)
        to_x = lax.rem(x + turn(band) * i + cols, NX)
        return owner_z * NX + to_x, delta, plane * NX + to_x

    def pack(i):
        for off in range(3):
            c, _, _ = route(i, off)
            j = off * cols + c
            for s in range(CAP):
                send[off, c, pl.ds(s, 6, stride=CAP), :] = part[sb_ref[s, j]]
            send[off, c, 36:37, :] = id_ref[pl.ds(j, 1), :]

    def transmit(i):
        for off in (0, 2, 1):
            c, delta, to = route(i, off)
            ok = to != col if off == 1 else valid(off)
            group = jnp.where(delta <= 1, 3 * delta, jnp.where(delta <= 4, 1, 2))

            @pl.when(ok)
            def _(off=off, c=c, delta=delta, to=to, group=group):
                pltpu.make_async_remote_copy(
                    src_ref=send.at[off, c, 0:SENT],
                    dst_ref=recv.at[delta * 3 * NX + (2 - off) * NX + x, 0:SENT],
                    send_sem=send_sem.at[off],
                    recv_sem=recv_sem.at[group, 2 - off],
                    device_id=(band + off - 1, to),
                    device_id_type=MESH,
                ).start()

    table_copy.wait()
    pack(0)
    inner = (band > 0).astype(jnp.int32) + (band < bands - 1).astype(jnp.int32)
    pl.semaphore_wait(barrier, cols - 1 + cols * inner)

    def both(i, carry):
        @pl.when(i < cols - 1)
        def _():
            pack(i + 1)

        transmit(i)
        return carry

    lax.fori_loop(0, cols, both, 0)
    mine = turn(band)
    up = lax.rem(z + mine + NZ, NZ) * NX + x
    down = lax.rem(z - mine + NZ, NZ) * NX + x
    down2 = lax.rem(z - 2 * mine + NZ, NZ) * NX + x
    for c, delta, group in ((col, 0, 0), (down, 1, 3), (down2, 2, 1), (up, 7, 2)):
        pltpu.make_async_copy(
            send.at[1, c, 0:SENT],
            recv.at[delta * 3 * NX + NX + x, 0:SENT],
            recv_sem.at[group, 1],
        ).start()
    data[...] = jnp.zeros_like(data)
    fill_base(base)
    fill_tables(base, table)

    def take(group):
        first, last = planes[group]
        n = (last - first) * NX
        for off in range(3):
            wait = pltpu.make_async_copy(recv.at[0:n, 0:SENT], recv.at[0:n, 0:SENT], recv_sem.at[group, off])
            if off == 1:
                wait.wait()
            else:

                @pl.when(valid(off))
                def _(wait=wait):
                    wait.wait()

    def summed(group, put):
        first, last = (3 * NX * p for p in planes[group])
        n = last - first

        def lay(i, carry):
            j = first + i
            for lev in range(6):
                data[pl.ds(pl.multiple_of(j * 8, 8), 6), 128 * lev : 128 * lev + 128] = recv[
                    j, lev * CAP : lev * CAP + CAP, :
                ]
            return carry

        lax.fori_loop(0, n, lay, 0)
        ids = recv[first:last, 36:37, :].reshape(n, 1, 128)
        lane = lax.broadcasted_iota(jnp.int32, (n, 8, 128), 2)
        sub = lax.broadcasted_iota(jnp.int32, (n, 8, 128), 1)
        diag = jnp.where(lane == sub, jnp.broadcast_to(ids, (n, 8, 128)), 0.0)
        diag = diag.reshape(8 * n, 128).astype(BF16)
        spread = jnp.dot(diag, jnp.ones((128, 128), BF16), preferred_element_type=F32)
        tile = lax.broadcasted_iota(jnp.int32, (8 * n, 128), 1).astype(F32)
        chooser = (spread == tile).astype(F32).astype(BF16)
        tn = (((0,), (0,)), ((), ()))
        for h in range(2):
            hi, lo = halves(data[8 * first : 8 * last, 384 * h : 384 * h + 384])
            put(
                h,
                lax.dot_general(chooser, hi, tn, preferred_element_type=F32)
                + lax.dot_general(chooser, lo, tn, preferred_element_type=F32),
            )

    def dense(which, h, to):
        return pltpu.make_async_remote_copy(
            src_ref=dtx.at[which, 3 * h : 3 * h + 3, 0:113],
            dst_ref=drx.at[which, 3 * h : 3 * h + 3, 0:113],
            send_sem=dense_sem.at[which, h, 0],
            recv_sem=dense_sem.at[which, h, 1],
            device_id=(band, to),
            device_id_type=MESH,
        )

    def keep(h, total):
        own[:, 384 * h : 384 * h + 384] = total

    def pass_on(which, to):
        def put(h, total):
            for lev in range(3):
                dtx[which, 3 * h + lev] = total[0:120, 128 * lev : 128 * lev + 128]
            dense(which, h, to).start()

        return put

    take(1)
    summed(1, pass_on(2, down))
    take(3)
    summed(3, keep)
    for h in range(2):
        dense(2, h, down).wait()
        for lev in range(3 * h, 3 * h + 3):
            dtx[0, lev] = own[0:120, 128 * lev : 128 * lev + 128] + drx[2, lev]
        dense(0, h, down).start()
    take(2)
    summed(2, pass_on(1, up))
    take(0)
    summed(0, keep)

    def row(lat):
        t, s = divmod(225 * lat, 128)
        a, b, c = (tiles[8 * (t + n) : 8 * (t + n) + 8, :] for n in range(3))
        if s:
            a, b, c = (pltpu.roll(v, 128 - s, 1) for v in (a, b, c))
            keep = lax.broadcasted_iota(jnp.int32, (8, 128), 1) < 128 - s
            a, b = jnp.where(keep, a, b), jnp.where(keep, b, c)
        return a, b

    def swap(src, dst, which, j):
        def step(i, carry):
            u = i // NX
            m = (u + 1) // 2
            dz = jnp.where(lax.rem(u, 2) == 0, 4 + m, 4 - m)
            to = lax.rem(z + dz, NZ) * NX + lax.rem(x + turn(band) * i + cols, NX)

            @pl.when(to != col)
            def _():
                pltpu.make_async_remote_copy(
                    src_ref=src.at[j, to, 0:12],
                    dst_ref=dst.at[j, col, 0:12],
                    send_sem=row_sem.at[which, j, 0],
                    recv_sem=row_sem.at[which, j, 1],
                    device_id=(band, to),
                    device_id_type=MESH,
                ).start()

            return carry

        lax.fori_loop(0, cols, step, 0)
        pltpu.make_async_copy(src.at[j, col, 0:12], dst.at[j, col, 0:12], row_sem.at[which, j, 1]).start()

    def swapped(dst, which, j):
        pltpu.make_async_copy(dst.at[j, :, 0:12], dst.at[j, :, 0:12], row_sem.at[which, j, 1]).wait()

    def swap_sent(src, which, j):
        part_of = src.at[j, 0 : cols - 1, 0:12]
        pltpu.make_async_copy(part_of, part_of, row_sem.at[which, j, 0]).wait()

    for h in range(2):
        dense(1, h, up).wait()
        dense(0, h, down).wait()
        for lev in range(3 * h, 3 * h + 3):
            tiles[pl.ds(lev, 120, stride=8), :] = (
                own[0:120, 128 * lev : 128 * lev + 128] + drx[0, lev] + drx[1, lev]
            )
        if h == 0:
            pl.semaphore_signal(
                pair_sem, inc=1, device_id=(band + turn(band), col), device_id_type=MESH
            )
        for lat in range(2 * cols):
            a, b = (v[3 * h : 3 * h + 3] for v in row(lat))
            flat[pl.ds(192 * h + lat, 3, stride=64), :] = a
            flat[pl.ds(384 + 192 * h + lat, 3, stride=64), :] = b
            first = 3 * (lat % 2)
            rtx[h, lat // 2, first : first + 3, :] = a
            rtx[h, lat // 2, 6 + first : 9 + first, :] = b
        if h == 0:
            pl.semaphore_wait(pair_sem, 1)
        swap(rtx, rrx, 0, h)
    out_ref[0, :, 0:128] = flat[0:384, :]
    out_ref[0, :, 128:225] = flat[384:768, 0:97]

    for j in range(2):
        swapped(rrx, 0, j)

        def get(c, j=j):
            return jnp.concatenate([rrx[j, c, 0:8, :], rrx[j, c, 6:14, :]], axis=1)

        def put(c, value, j=j):
            ztx[j, c, 0:6, :] = value[0:6, 0:128]
            ztx[j, c, 6:12, :] = value[0:6, 128:256]

        zonal(get, put, table, (pick_ref[6, 0], pick_ref[6, 1]))
        swap(ztx, zrx, 1, j)

    pltpu.make_async_copy(
        send.at[1, 0 : cols - 4, 0:SENT], send.at[1, 0 : cols - 4, 0:SENT], send_sem.at[1]
    ).wait()
    for off in (0, 2):

        @pl.when(valid(off))
        def _(off=off):
            pltpu.make_async_copy(send.at[off, :, 0:SENT], send.at[off, :, 0:SENT], send_sem.at[off]).wait()

    for j in range(2):
        swap_sent(rtx, 0, j)
    for j in range(2):
        swapped(zrx, 1, j)
        for lat in range(2 * cols):
            first = 3 * (lat % 2)
            flat[pl.ds(192 * j + lat, 3, stride=64), :] = zrx[j, lat // 2, first : first + 3, :]
            flat[pl.ds(384 + 192 * j + lat, 3, stride=64), :] = zrx[j, lat // 2, 6 + first : 9 + first, :]
    out_ref[1, :, 0:128] = flat[0:384, :]
    out_ref[1, :, 128:225] = flat[384:768, 0:97]
    for j in range(2):
        swap_sent(ztx, 1, j)


def local(source, weights, source_block, owner_device, target_tile, cutoff):
    cols = lax.axis_size("col")
    levels, nb, width = 6, weights.shape[0], weights.shape[1]
    blocks = jnp.transpose(source.reshape(levels, -1, width), (1, 0, 2))
    spare = jnp.zeros((nb - cutoff.shape[0],), jnp.int32)
    meta = jnp.concatenate([owner_device[:, 0], target_tile, source_block, cutoff, spare]).reshape(8, nb // 2)
    vmem = pl.BlockSpec(memory_space=pltpu.VMEM)
    rows = (2, cols, 16, 128)
    both = pl.pallas_call(
        kernel,
        name="remap",
        out_shape=jax.ShapeDtypeStruct((2, 384, 225), F32),
        in_specs=[vmem, vmem, pl.BlockSpec(memory_space=pl.ANY)],
        out_specs=vmem,
        scratch_shapes=[
            pltpu.SMEM((8, nb // 2), jnp.int32),
            pltpu.VMEM((8, 128), jnp.int32),
            pltpu.SMEM((8, 128), jnp.int32),
            pltpu.VMEM((128, 128), F32),
            pltpu.VMEM((nb, width, width), BF16),
            pltpu.VMEM((nb, 6, 128), F32),
            pltpu.VMEM((3, cols, ROWS, 128), F32),
            pltpu.VMEM((3 * cols, ROWS, 128), F32),
            pltpu.VMEM((24 * cols, 768), F32),
            pltpu.VMEM((128, 768), F32),
            pltpu.VMEM((3, 6, 120, 128), F32),
            pltpu.VMEM((3, 6, 120, 128), F32),
            pltpu.VMEM((1024, 128), F32),
            pltpu.VMEM((768, 128), F32),
            pltpu.VMEM(rows, F32),
            pltpu.VMEM(rows, F32),
            pltpu.VMEM(rows, F32),
            pltpu.VMEM(rows, F32),
            pltpu.VMEM((112, 256), F32),
            pltpu.VMEM((2, 17, 64, 512), BF16),
            pltpu.SemaphoreType.DMA((2,)),
            pltpu.SemaphoreType.DMA((nb // GROUP,)),
            pltpu.SemaphoreType.DMA((3,)),
            pltpu.SemaphoreType.DMA((4, 3)),
            pltpu.SemaphoreType.DMA((3, 2, 2)),
            pltpu.SemaphoreType.DMA((2, 2, 2)),
            pltpu.SemaphoreType.REGULAR,
        ],
        compiler_params=pltpu.CompilerParams(
            collective_id=0, has_side_effects=True, vmem_limit_bytes=50 * 2**20
        ),
    )(meta, blocks, weights)
    return both[0].reshape(6, 64, 225), both[1].reshape(6, 64, 225)


def solution(mesh):
    in_specs = (
        P(None, ("band", "col")),
        P(("band", "col"), None, None),
        P(("band", "col")),
        P(("band", "col"), None),
        P(("band", "col")),
        P(("band", "col")),
    )
    out_specs = (P(None, "band", "col"), P(None, "band", "col"))
    return jax.shard_map(local, mesh=mesh, in_specs=in_specs, out_specs=out_specs, check_vma=False)
```
